32 devices in a mesh: grp: 4 (over z), seq: 8 (over y, x, core).
Axes of the slice: x: 2, y: 2, z: 4, core: 2. Of those that a mesh axis runs over, the one named last changes fastest.
Arguments:
- hist_keys: bfloat16 [4, 1024, 1024], P('grp', 'seq'), may hold values from -4 to 4
- hist_values: bfloat16 [4, 1024, 1024], P('grp', 'seq'), may hold values from -6 to 6
- latent_queries: bfloat16 [4, 64, 1024], P('grp', 'seq'), may hold values from -48 to 48
- latent_pos: int32 [4, 64], P('grp'), may hold values from 128 to 1023
- targets: int32 [4, 64], P('grp', 'seq'), may hold values from 0 to 127
- out_proj: bfloat16 [1024, 2048], P('seq'), may hold values from -0.1875 to 0.1875
- norm_gain: float32 [2048], replicated, may hold values from 0.1 to 1.9
- unembed: bfloat16 [2048, 128], replicated, may hold values from -0.125 to 0.125
Outputs:
- loss: float32 [4], P('grp')
- grad_queries: bfloat16 [4, 64, 1024], P('grp', 'seq')
- grad_keys: bfloat16 [4, 1024, 1024], P('grp', 'seq')
- grad_values: bfloat16 [4, 1024, 1024], P('grp', 'seq')
- proj_update: float32 [1024, 2048], P('seq')
The draws below stay inside these ranges and needn't reach their ends.
All inputs are finite; a program needn't handle non-finite values.
Results may differ from the reference program's by a relative error of at most 0.03.
Values may be sent and summed in bfloat16 or wider, within the bound.
No kernel may reach another device: no remote copies, remote signals or barrier semaphores. Data moves between devices by JAX's collectives and lax.ppermute only.
A program may use at most 64 MiB of HBM per device.

```python
import math
import jax
import jax.numpy as jnp
import numpy as np
from jax import lax

D = 2048
HEADS = 8
HD = 128
VOCAB = 128
NL = 64
TOK_DEV = 128
HC = 1024
LENGTH = 1024
SEQS = 4
N_SEQ = 8


def shared_keys(key):
    base = jax.random.fold_in(key, 7)
    first = jax.random.fold_in(base, 0)
    channels = HEADS * HD
    keys_all = jnp.clip(jax.random.normal(first, (SEQS, LENGTH, channels), jnp.float32), -4.0, 4.0)
    return keys_all


def draw_hist_keys(key, part):
    keys_all = shared_keys(key)
    return keys_all.astype(jnp.bfloat16)


def draw_latent_queries(key, part):
    own_key = jax.random.fold_in(key, 11)
    first = jax.random.fold_in(own_key, 0)
    queries = jnp.clip(jax.random.normal(first, (SEQS, NL, HEADS * HD), jnp.float32), -4.0, 4.0)
    return queries.astype(jnp.bfloat16)


def with_ends(values, stream_key, least, top_value):
    longest = values.shape.index(max(values.shape))
    spots = []
    for shift in (0, 1):
        where = [jax.random.randint(jax.random.fold_in(stream_key, axis), (), 0, length) for axis, length in enumerate(values.shape)]
        where[longest] = (where[longest] + shift) % values.shape[longest]
        spots.append(tuple(where))
    return values.at[spots[0]].set(least).at[spots[1]].set(top_value)


def levels(key, dims, pieces, least, top_value):
    def one(dim, shards_of):
        heights = jax.random.uniform(jax.random.fold_in(jax.random.fold_in(key, 6), dim), (shards_of,), jnp.float32, least / len(pieces), top_value / len(pieces))
        return jnp.repeat(jnp.exp(heights), dims[dim] // shards_of).reshape((-1,) + (1,) * (len(dims) - dim - 1))

    loudness = one(*pieces[0])
    for cut in pieces[1:]:
        loudness = loudness * one(*cut)
    return loudness


def cumulative_ranks(count, slope):
    weights = [(1 << 20) // math.isqrt(rank ** slope) + 1 for rank in range(1, count + 1)]
    deviation = 1 + sum(weights) // (1 << 30)
    return np.cumsum(np.array([max(1, weight // deviation) for weight in weights]))


def ranked(key, dims, count, skew):
    listing = cumulative_ranks(count, skew)
    pick = jax.random.randint(jax.random.fold_in(key, 1), dims, 0, int(listing[count - 1]))
    grade = jnp.searchsorted(jnp.asarray(listing, jnp.int32), pick, side="right")
    return jax.random.permutation(jax.random.fold_in(key, 2), count)[grade].astype(jnp.int32)


def bell_draw(key, extent, deviation, limit, cuts=(), held_as=jnp.bfloat16):
    result = jax.random.normal(key, extent, jnp.float32) * deviation
    if len(cuts) > 0:
        result = levels(key, extent, cuts, -0.22, 0.18) * result
    return jnp.clip(result, min=-limit, max=limit).astype(held_as)


def setup_inputs(seed: int = 0) -> dict:
    seeds = jax.random.split(jax.random.key(seed), 9)
    return {
        "hist_keys": draw_hist_keys(jax.random.fold_in(seeds[8], 71), 0),
        "hist_values": bell_draw(seeds[1], (SEQS, LENGTH, HC), 1.0, 6.0, ((0, 4), (1, 8))),
        "latent_queries": draw_latent_queries(jax.random.fold_in(seeds[8], 71), 0),
        "latent_pos": with_ends(jax.random.randint(seeds[3], (SEQS, NL), LENGTH // 8, LENGTH), jax.random.fold_in(seeds[3], 1), LENGTH // 8, LENGTH - 1).astype(jnp.int32),
        "targets": with_ends(ranked(seeds[4], (SEQS, NL), VOCAB, 2), jax.random.fold_in(seeds[4], 3), 0, VOCAB - 1).astype(jnp.int32),
        "out_proj": bell_draw(seeds[5], (HC, D), HC ** -0.5, 0.1875, ((0, 8),)),
        "norm_gain": jnp.clip(1.0 + 0.18 * jax.random.normal(seeds[6], (D,), jnp.float32), 0.1, 1.9),
        "unembed": bell_draw(seeds[7], (D, VOCAB), D ** -0.5, 0.125),
    }


epsilon = 1e-06
loss_factor = 64.0

def head_split(array):
    return array.reshape(array.shape[0], -1, HD)

def reference(hist_keys, hist_values, latent_queries, latent_pos, targets, out_proj, norm_gain, unembed):
    softmax_scale = HD ** (-0.5)
    channels = HEADS * HD
    block_starts = jnp.arange(N_SEQ, dtype=jnp.int32) * TOK_DEV

    def one_sequence(carried, inputs):
        seq_keys, seq_values, seq_queries, positions, seq_targets = inputs
        query_heads = head_split(seq_queries.astype(jnp.float32))
        key_blocks = seq_keys.reshape(N_SEQ, TOK_DEV, channels)
        value_blocks = seq_values.reshape(N_SEQ, TOK_DEV, channels)

        def block_scores(block_keys, block_start):
            scores = jnp.einsum('ihd,jhd->hij', query_heads, head_split(block_keys.astype(jnp.float32))) * softmax_scale
            places = block_start + jnp.arange(TOK_DEV, dtype=jnp.int32)
            visible = (places[None, :] <= positions[:, None])[None]
            return (scores, visible)

        def forward_block(block_inputs):
            block_keys, block_values, block_start = block_inputs
            scores, visible = block_scores(block_keys, block_start)
            largest = lax.optimization_barrier(jnp.max(jnp.where(visible, scores, -1e+30), axis=-1))
            weights = jnp.where(visible, jnp.exp(scores - largest[..., None]), 0.0)
            summed = lax.optimization_barrier(jnp.sum(weights, axis=-1))
            rounded = weights.astype(jnp.bfloat16).astype(jnp.float32)
            partial_out = jnp.einsum('hij,jhd->ihd', rounded, head_split(block_values.astype(jnp.float32)))
            return (largest.T, summed.T, partial_out.reshape(NL, channels))
        maxima, sums, partials = lax.map(forward_block, (key_blocks, value_blocks, block_starts))
        best = lax.optimization_barrier(jnp.max(maxima, axis=0))
        factors = jnp.exp(maxima - best)
        denom = lax.optimization_barrier(jnp.sum(sums * factors, axis=0))
        combined = lax.optimization_barrier(jnp.sum(partials * jnp.repeat(factors, HD, axis=-1), axis=0))
        attn = (combined / jnp.repeat(denom, HD, axis=-1)).astype(jnp.bfloat16)
        log_norm = best + jnp.log(denom)
        hidden = jnp.dot(attn, out_proj, preferred_element_type=jnp.float32)
        inverse = lax.rsqrt(lax.optimization_barrier(jnp.mean(hidden * hidden, axis=-1, keepdims=True)) + epsilon)
        normed = (hidden * inverse * norm_gain).astype(jnp.bfloat16)
        logits = jnp.dot(normed, unembed, preferred_element_type=jnp.float32)
        log_total = jax.nn.logsumexp(logits, axis=-1, keepdims=True)
        onehot = (jnp.arange(VOCAB, dtype=jnp.int32)[None, :] == seq_targets[:, None]).astype(jnp.float32)
        seq_loss = jnp.sum(log_total[:, 0] - lax.optimization_barrier(jnp.sum(logits * onehot, axis=-1)))
        grad_logits = (loss_factor * (jnp.exp(logits - log_total) - onehot)).astype(jnp.bfloat16)
        grad_normed = jnp.dot(grad_logits, unembed.T, preferred_element_type=jnp.float32)
        scaled = norm_gain * grad_normed
        grad_hidden = (inverse * scaled - hidden * inverse ** 3 * lax.optimization_barrier(jnp.mean(hidden * scaled, axis=-1, keepdims=True))).astype(jnp.bfloat16)
        weight_grad = jnp.dot(attn.T, grad_hidden, preferred_element_type=jnp.float32)
        grad_attn = jnp.dot(grad_hidden, out_proj.T, preferred_element_type=jnp.float32).astype(jnp.bfloat16)
        grad_heads = head_split(grad_attn.astype(jnp.float32))
        delta = lax.optimization_barrier(jnp.sum(grad_heads * head_split(attn.astype(jnp.float32)), axis=-1))

        def backward_block(block_inputs):
            block_keys, block_values, block_start = block_inputs
            scores, visible = block_scores(block_keys, block_start)
            probs = jnp.where(visible, jnp.exp(scores - log_norm.T[..., None]), 0.0)
            probs_low = probs.astype(jnp.bfloat16).astype(jnp.float32)
            value_heads = head_split(block_values.astype(jnp.float32))
            grad_probs = jnp.einsum('ihd,jhd->hij', grad_heads, value_heads)
            grad_scores = (probs * (grad_probs - delta.T[..., None])).astype(jnp.bfloat16).astype(jnp.float32)
            grad_v = jnp.einsum('hij,ihd->jhd', probs_low, grad_heads).reshape(TOK_DEV, channels).astype(jnp.bfloat16)
            grad_k = (jnp.einsum('hij,ihd->jhd', grad_scores, query_heads) * softmax_scale).reshape(TOK_DEV, channels).astype(jnp.bfloat16)
            grad_q = jnp.einsum('hij,jhd->ihd', grad_scores, head_split(block_keys.astype(jnp.float32))).reshape(NL, channels) * softmax_scale
            return (grad_k, grad_v, grad_q)
        grad_k, grad_v, grad_q = lax.map(backward_block, (key_blocks, value_blocks, block_starts))
        outputs = (seq_loss, lax.optimization_barrier(jnp.sum(grad_q, axis=0)).astype(jnp.bfloat16), grad_k.reshape(N_SEQ * TOK_DEV, channels), grad_v.reshape(N_SEQ * TOK_DEV, channels))
        return (carried + weight_grad, outputs)
    start_grad = jnp.zeros((HEADS * HD, D), jnp.float32)
    weight_total, results = lax.scan(one_sequence, start_grad, (hist_keys, hist_values, latent_queries, latent_pos, targets))
    losses, grad_queries, grad_keys, grad_values = results
    proj_update = weight_total * lax.rsqrt(jnp.mean(weight_total * weight_total) + epsilon)
    return (losses, grad_queries, grad_keys, grad_values, proj_update)
```

```python
from functools import partial

import jax
import jax.numpy as jnp
from jax import lax
from jax.experimental import pallas as pl
from jax.experimental.pallas import tpu as pltpu
from jax.sharding import PartitionSpec as P

D = 2048
HD = 128


epsilon = 1e-06
loss_factor = 64.0


def joined(part, axis, combine):
    gathered = jax.tree.map(lambda a: lax.all_gather(a, axis), part)

    def take(source):
        return jax.tree.map(lambda a: lax.dynamic_index_in_dim(a, source, 0, False), gathered)

    return lax.fori_loop(
        1, lax.axis_size(axis), lambda source, state: combine(state, take(source)), take(0)
    )


def repeat_heads(stat):
    return jnp.repeat(stat, HD, axis=-1)


def combine(earlier, later):
    best = jnp.maximum(earlier[0], later[0])
    factor_one = jnp.exp(earlier[0] - best)
    factor_two = jnp.exp(later[0] - best)
    denom = earlier[1] * factor_one + later[1] * factor_two
    summed = earlier[2] * repeat_heads(factor_one) + later[2] * repeat_heads(factor_two)
    return (best, denom, summed)


def general_body(hist_keys, hist_values, latent_queries, latent_pos, targets, out_proj, norm_gain, unembed):
    softmax_scale = HD ** (-0.5)
    seq_keys = hist_keys[0]
    seq_values = hist_values[0]
    position = lax.axis_index("seq")
    tok_rows = seq_keys.shape[0]
    channels = seq_keys.shape[1]
    head_count = channels // HD
    own_rows = latent_queries.shape[1]
    queries = lax.all_gather(latent_queries[0], "seq", axis=0, tiled=True)
    latents = queries.shape[0]
    query_heads = queries.reshape(latents, head_count, HD)
    key_heads = seq_keys.reshape(tok_rows, head_count, HD)
    value_heads = seq_values.reshape(tok_rows, head_count, HD)
    places = position * tok_rows + jnp.arange(tok_rows, dtype=jnp.int32)
    visible = (places[None, :] <= latent_pos[0][:, None])[None]
    scores = (
        jnp.einsum("ihd,jhd->hij", query_heads, key_heads, preferred_element_type=jnp.float32)
        * softmax_scale
    )
    largest = jnp.max(jnp.where(visible, scores, -1e30), axis=-1)
    weights = jnp.where(visible, jnp.exp(scores - largest[..., None]), 0.0)
    summed = jnp.sum(weights, axis=-1)
    partial_out = jnp.einsum(
        "hij,jhd->ihd",
        weights.astype(jnp.bfloat16),
        value_heads,
        preferred_element_type=jnp.float32,
    ).reshape(latents, channels)
    best, denom, combined = joined((largest.T, summed.T, partial_out), "seq", combine)
    attn_all = (combined / repeat_heads(denom)).astype(jnp.bfloat16)
    log_norm = best + jnp.log(denom)
    slab = out_proj.shape[0]
    attn_cols = lax.dynamic_slice_in_dim(attn_all, position * slab, slab, 1)
    proj_columns = lax.all_to_all(out_proj, "seq", split_axis=1, concat_axis=0, tiled=True)
    column_block = jnp.dot(attn_all, proj_columns, preferred_element_type=jnp.float32)
    hidden = lax.all_to_all(column_block, "seq", split_axis=0, concat_axis=1, tiled=True)
    inverse = lax.rsqrt(jnp.mean(hidden * hidden, axis=-1, keepdims=True) + epsilon)
    normed = (hidden * inverse * norm_gain).astype(jnp.bfloat16)
    logits = jnp.dot(normed, unembed, preferred_element_type=jnp.float32)
    log_total = jax.nn.logsumexp(logits, axis=-1, keepdims=True)
    onehot = (jnp.arange(logits.shape[1], dtype=jnp.int32)[None, :] == targets[0][:, None]).astype(
        jnp.float32
    )
    local_loss = jnp.sum(log_total[:, 0] - jnp.sum(logits * onehot, axis=-1))
    grad_logits = (loss_factor * (jnp.exp(logits - log_total) - onehot)).astype(jnp.bfloat16)
    grad_normed = lax.dot_general(
        grad_logits, unembed, (((1,), (1,)), ((), ())), preferred_element_type=jnp.float32
    )
    scaled = norm_gain * grad_normed
    grad_hidden = (
        inverse * scaled - hidden * inverse**3 * jnp.mean(hidden * scaled, axis=-1, keepdims=True)
    ).astype(jnp.bfloat16)
    grad_all = lax.all_gather(grad_hidden, "seq", axis=0, tiled=True)
    weight_part = lax.dot_general(
        attn_cols, grad_all, (((0,), (0,)), ((), ())), preferred_element_type=jnp.float32
    )
    grad_cols = lax.dot_general(
        grad_all, out_proj, (((1,), (1,)), ((), ())), preferred_element_type=jnp.float32
    ).astype(jnp.bfloat16)
    grad_attn = lax.all_gather(grad_cols, "seq", axis=1, tiled=True)
    grad_heads = grad_attn.reshape(latents, head_count, HD)
    product = grad_attn.astype(jnp.float32) * attn_all.astype(jnp.float32)
    delta = jnp.sum(product.reshape(latents, head_count, HD), axis=-1)
    probs = jnp.where(visible, jnp.exp(scores - log_norm.T[..., None]), 0.0)
    grad_probs = jnp.einsum(
        "ihd,jhd->hij", grad_heads, value_heads, preferred_element_type=jnp.float32
    )
    grad_scores = (probs * (grad_probs - delta.T[..., None])).astype(jnp.bfloat16)
    grad_values = (
        jnp.einsum(
            "hij,ihd->jhd",
            probs.astype(jnp.bfloat16),
            grad_heads,
            preferred_element_type=jnp.float32,
        )
        .reshape(tok_rows, channels)
        .astype(jnp.bfloat16)
    )
    grad_keys = (
        (
            jnp.einsum("hij,ihd->jhd", grad_scores, query_heads, preferred_element_type=jnp.float32)
            * softmax_scale
        )
        .reshape(tok_rows, channels)
        .astype(jnp.bfloat16)
    )
    terms = jnp.einsum("hij,jhd->ihd", grad_scores, key_heads, preferred_element_type=jnp.float32)
    grad_queries = lax.psum_scatter(
        (terms.reshape(lax.axis_size("seq") * own_rows, channels) * softmax_scale).astype(
            jnp.bfloat16
        ),
        "seq",
        scatter_dimension=0,
        tiled=True,
    )
    entries = channels * D
    weight_sum = lax.psum(weight_part.astype(jnp.bfloat16), "grp").astype(jnp.float32)
    loss_sum, square_sum = lax.psum((local_loss, jnp.sum(weight_sum * weight_sum)), "seq")
    proj_update = weight_sum * lax.rsqrt(square_sum / entries + epsilon)
    return (
        loss_sum.reshape(1),
        grad_queries[None],
        grad_keys[None],
        grad_values[None],
        proj_update,
    )


VMEM = pl.BlockSpec(memory_space=pltpu.VMEM)
SMEM = pl.BlockSpec(memory_space=pltpu.SMEM)
ROWS_T = (((1,), (1,)), ((), ()))
COLS_T = (((0,), (0,)), ((), ()))


def matmul(one, two, dims=(((1,), (0,)), ((), ()))):
    return lax.dot_general(one, two, dims, preferred_element_type=jnp.float32)


def kernel_call(kernel, name, in_specs, outs, scratch=()):
    return pl.pallas_call(
        kernel,
        name=name,
        in_specs=in_specs,
        out_specs=[VMEM] * len(outs),
        out_shape=[jax.ShapeDtypeStruct(shape, dtype) for shape, dtype in outs],
        scratch_shapes=list(scratch),
    )


def pack_kernel(targets, keys, values, queries, packed):
    heads = packed.shape[0]
    tok = keys.shape[0]
    own = queries.shape[0]
    lanes = lax.broadcasted_iota(jnp.int32, (own, HD), 1)
    rows = lax.broadcasted_iota(jnp.int32, (own, HD), 0)
    wanted = jnp.zeros((own, HD), jnp.int32)
    for row in range(own):
        wanted = jnp.where(rows == row, targets[0, row], wanted)
    onehot = (lanes == wanted).astype(jnp.float32)
    for head in range(heads):
        cols = slice(head * HD, (head + 1) * HD)
        packed[head, 0:tok, :] = keys[:, cols]
        packed[head, tok : 2 * tok, :] = values[:, cols]
        tail = jnp.concatenate([queries[:, cols].astype(jnp.float32), onehot], axis=0)
        packed[head, 2 * tok : 2 * tok + 2 * own, :] = tail.astype(jnp.bfloat16)


def split_packed(packed, tok, own):
    heads = packed.shape[0]
    keys = packed[:, 0:tok, :].reshape(heads * tok, HD)
    values = packed[:, tok : 2 * tok, :].reshape(heads * tok, HD)
    queries = packed[:, 2 * tok : 2 * tok + own, :].astype(jnp.float32).reshape(heads * own, HD)
    return keys, values, queries.astype(jnp.bfloat16)


def visible_scores(keys, queries, positions):
    latents = queries.shape[0]
    length = keys.shape[0]
    diagonal = lax.broadcasted_iota(jnp.int32, (latents, latents), 0) == lax.broadcasted_iota(
        jnp.int32, (latents, latents), 1
    )
    last = jnp.sum(
        jnp.where(diagonal, positions[...].astype(jnp.float32), 0.0), axis=1, keepdims=True
    )
    places = lax.broadcasted_iota(jnp.int32, (latents, length), 1).astype(jnp.float32)
    scores = matmul(queries, keys, ROWS_T) * HD ** (-0.5)
    return scores, places <= last


def forward_kernel(side, positions, packed, out_proj, attn, log_norm, onehot, kept, sent, *, tok, own):
    keys, values, queries = split_packed(packed, tok, own)
    scores, visible = visible_scores(keys, queries, positions)
    best = jnp.max(jnp.where(visible, scores, -1e30), axis=-1, keepdims=True)
    weights = jnp.where(visible, jnp.exp(scores - best), 0.0)
    denom = jnp.sum(weights, axis=-1, keepdims=True)
    summed = matmul(weights.astype(jnp.bfloat16), values)
    attn[...] = (summed / denom).astype(jnp.bfloat16)
    log_norm[...] = jnp.broadcast_to(best + jnp.log(denom), log_norm.shape)
    half = kept.shape[0]
    mine = side[0]
    pieces = half // own
    onehot[...] = (
        packed[pl.ds(mine * pieces, pieces), 2 * tok + own : 2 * tok + 2 * own, :]
        .astype(jnp.float32)
        .reshape(half, HD)
    )
    proj = out_proj[...]
    kept[...] = matmul(attn[pl.ds(pl.multiple_of(mine * half, half), half), :], proj)
    sent[...] = matmul(attn[pl.ds(pl.multiple_of((1 - mine) * half, half), half), :], proj).astype(
        sent.dtype
    )


def loss_kernel(parts, gain, unembed, onehot_ref, attn, message, stats):
    half = parts.shape[1]
    hidden = parts[0].astype(jnp.float32)
    for part in range(1, parts.shape[0]):
        hidden = hidden + parts[part].astype(jnp.float32)
    onehot = onehot_ref[...]
    inverse = lax.rsqrt(jnp.mean(hidden * hidden, axis=-1, keepdims=True) + epsilon)
    normed = (hidden * inverse * gain[...]).astype(jnp.bfloat16)
    logits = matmul(normed, unembed[...])
    top = jnp.max(logits, axis=-1, keepdims=True)
    log_total = top + jnp.log(jnp.sum(jnp.exp(logits - top), axis=-1, keepdims=True))
    losses = log_total - jnp.sum(logits * onehot, axis=-1, keepdims=True)
    stats[...] = jnp.broadcast_to(jnp.sum(losses, axis=0, keepdims=True), stats.shape)
    grad_logits = (loss_factor * (jnp.exp(logits - log_total) - onehot)).astype(jnp.bfloat16)
    scaled = gain[...] * matmul(grad_logits, unembed[...], ROWS_T)
    mean = jnp.mean(hidden * scaled, axis=-1, keepdims=True)
    grad_hidden = (inverse * scaled - hidden * (inverse * inverse * inverse) * mean).astype(
        jnp.bfloat16
    )
    blocks = hidden.shape[1] // HD
    for block in range(blocks):
        message[block * half : (block + 1) * half, :] = grad_hidden[:, block * HD : (block + 1) * HD]
    message[blocks * half :, :] = attn[...]


def fill_rows(target, row, message, half):
    for block in range(target.shape[1] // HD):
        target[pl.ds(row, half), block * HD : (block + 1) * HD] = message[
            block * half : (block + 1) * half, :
        ]


def backward_kernel(
    side, positions, packed, out_proj, attn, log_norm, own_msg, pair_msg, grads, grad_hidden, *, tok, own
):
    half = grad_hidden.shape[0] // 2
    mine = side[0]
    fill_rows(grad_hidden, pl.multiple_of(mine * half, half), own_msg, half)
    fill_rows(grad_hidden, pl.multiple_of((1 - mine) * half, half), pair_msg, half)
    keys, values, queries = split_packed(packed, tok, own)
    scores, visible = visible_scores(keys, queries, positions)
    heads = packed.shape[0]
    grad_attn = matmul(grad_hidden[...], out_proj[...], ROWS_T).astype(jnp.bfloat16)
    delta = jnp.sum(
        grad_attn.astype(jnp.float32) * attn[...].astype(jnp.float32), axis=-1, keepdims=True
    )
    probs = jnp.where(visible, jnp.exp(scores - log_norm[:, 0:1]), 0.0)
    grad_probs = matmul(grad_attn, values, ROWS_T)
    grad_scores = (probs * (grad_probs - delta)).astype(jnp.bfloat16)
    grad_values = matmul(probs.astype(jnp.bfloat16), grad_attn, COLS_T).astype(jnp.bfloat16)
    scale = HD ** (-0.5)
    grad_keys = (matmul(grad_scores, queries, COLS_T) * scale).astype(jnp.bfloat16)
    grad_queries = matmul(grad_scores, keys) * scale
    grads[:, 0:tok, :] = grad_keys.reshape(heads, tok, HD)
    grads[:, tok : 2 * tok, :] = grad_values.reshape(heads, tok, HD)
    tail = grad_queries.reshape(heads, own, HD)
    grads[:, 2 * tok : 2 * tok + 2 * own, :] = jnp.concatenate([tail, tail], axis=1).astype(
        jnp.bfloat16
    )


def unpack_kernel(packed, grad_queries, grad_keys, grad_values):
    heads = packed.shape[0]
    tok = grad_keys.shape[0]
    own = grad_queries.shape[0]
    for head in range(heads):
        cols = slice(head * HD, (head + 1) * HD)
        grad_keys[:, cols] = packed[head, 0:tok, :]
        grad_values[:, cols] = packed[head, tok : 2 * tok, :]
        grad_queries[:, cols] = packed[head, 2 * tok : 2 * tok + own, :]


def weight_kernel(side, *refs, count):
    messages = refs[: 2 * count]
    loss, weights, stats, attn_rows, grad_rows = refs[2 * count :]
    half = grad_rows.shape[0] // (2 * count)
    blocks = grad_rows.shape[1] // HD
    mine = side[0]
    for index in range(count):
        attn_at = blocks * half
        for place, message, part in (
            (0, messages[index], mine),
            (1, messages[count + index], 1 - mine),
        ):
            row = (2 * index + place) * half
            for block in range(blocks):
                grad_rows[row : row + half, block * HD : (block + 1) * HD] = message[
                    block * half : (block + 1) * half, :
                ]
            attn_rows[row : row + half, :] = messages[index][
                pl.ds(pl.multiple_of(attn_at + part * half, half), half), :
            ]
    total = matmul(attn_rows[...], grad_rows[...], COLS_T)
    weights[...] = total
    squares = jnp.sum(jnp.sum(total * total, axis=0, keepdims=True), axis=1, keepdims=True)
    lanes = lax.broadcasted_iota(jnp.int32, stats.shape, 1)
    stats[...] = jnp.where(lanes < HD // 2, squares, loss[...])


def body(hist_keys, hist_values, latent_queries, latent_pos, targets, out_proj, norm_gain, unembed):
    n_seq = lax.axis_size("seq")
    n_grp = lax.axis_size("grp")
    seq_keys = hist_keys[0]
    tok, channels = seq_keys.shape
    own = latent_queries.shape[1]
    latents = n_seq * own
    heads = channels // HD
    vocab = unembed.shape[1]
    if not (
        heads == n_seq
        and out_proj.shape[0] == HD
        and vocab == HD
        and tok % 16 == 0
        and own == 8
        and n_seq % 2 == 0
    ):
        return general_body(
            hist_keys, hist_values, latent_queries, latent_pos, targets, out_proj, norm_gain, unembed
        )
    bf16, f32 = jnp.bfloat16, jnp.float32
    half = latents // 2
    width = out_proj.shape[1]
    span = 2 * tok + 2 * own
    side = (lax.axis_index("seq") % 2).reshape(1)
    swap = [(i, i ^ 1) for i in range(n_seq)]
    sides = [[i for i in range(n_seq) if i % 2 == k] for k in range(2)]

    (packed,) = kernel_call(
        pack_kernel, "pack", [SMEM, VMEM, VMEM, VMEM], [((heads, span, HD), bf16)]
    )(targets, seq_keys, hist_values[0], latent_queries[0])
    packed = lax.all_to_all(packed, "seq", 0, 0)

    attn, log_norm, onehot, kept, sent = kernel_call(
        partial(forward_kernel, tok=tok, own=own),
        "forward",
        [SMEM, VMEM, VMEM, VMEM],
        [
            ((latents, HD), bf16),
            ((latents, HD), f32),
            ((half, HD), f32),
            ((half, width), f32),
            ((half, width), bf16),
        ],
    )(side, latent_pos, packed, out_proj)
    pair_sum = (kept + lax.ppermute(sent, "seq", swap).astype(f32)).astype(bf16)
    parts = lax.all_gather(pair_sum, "seq", axis_index_groups=sides)
    message, loss = kernel_call(
        loss_kernel,
        "loss",
        [VMEM] * 5,
        [((width // HD * half + latents, HD), bf16), ((1, HD), f32)],
    )(parts, norm_gain.reshape(1, width), unembed, onehot, attn)
    pair_msg = lax.ppermute(message, "seq", swap)
    others = [
        lax.ppermute(message, "grp", [(i, (i + step) % n_grp) for i in range(n_grp)])
        for step in range(1, n_grp)
    ]
    (grads,) = kernel_call(
        partial(backward_kernel, tok=tok, own=own),
        "backward",
        [SMEM] + [VMEM] * 7,
        [((heads, span, HD), bf16)],
        [pltpu.VMEM((latents, width), bf16)],
    )(side, latent_pos, packed, out_proj, attn, log_norm, message, pair_msg)
    grads = lax.all_to_all(grads, "seq", 0, 0)
    pair_others = [lax.ppermute(other, "seq", swap) for other in others]
    weights, stats = kernel_call(
        partial(weight_kernel, count=n_grp),
        "weights",
        [SMEM] + [VMEM] * (2 * n_grp + 1),
        [((channels // n_seq, width), f32), ((1, HD), f32)],
        [
            pltpu.VMEM((n_grp * latents, HD), bf16),
            pltpu.VMEM((n_grp * latents, width), bf16),
        ],
    )(side, message, *others, pair_msg, *pair_others, loss)
    grad_queries, grad_keys, grad_values = kernel_call(
        unpack_kernel,
        "unpack",
        [VMEM],
        [((own, channels), bf16), ((tok, channels), bf16), ((tok, channels), bf16)],
    )(grads)
    gathered = lax.all_gather(stats, "seq", axis=0, tiled=True)
    totals = jnp.sum(gathered, axis=0)
    loss_sum = totals[HD - 1] / (n_seq // 2)
    proj_update = weights * lax.rsqrt(totals[0] / (channels * width) + epsilon)
    return (
        loss_sum.reshape(1),
        grad_queries[None],
        grad_keys[None],
        grad_values[None],
        proj_update,
    )


def solution(mesh):
    placed = (
        P("grp", "seq", None),
        P("grp", "seq", None),
        P("grp", "seq", None),
        P("grp", None),
        P("grp", "seq"),
        P("seq", None),
        P(),
        P(),
    )
    return jax.shard_map(
        body,
        mesh=mesh,
        in_specs=placed,
        out_specs=(
            P("grp"),
            P("grp", "seq", None),
            P("grp", "seq", None),
            P("grp", "seq", None),
            P("seq", None),
        ),
        check_vma=False,
    )
```

```python
from functools import partial

import jax
import jax.numpy as jnp
from jax import lax
from jax.experimental import pallas as pl
from jax.experimental.pallas import tpu as pltpu
from jax.sharding import PartitionSpec as P


D = 2048
HD = 128


epsilon = 1e-06
loss_factor = 64.0


def joined(part, axis, combine):
    gathered = jax.tree.map(lambda a: lax.all_gather(a, axis), part)

    def take(source):
        return jax.tree.map(lambda a: lax.dynamic_index_in_dim(a, source, 0, False), gathered)

    return lax.fori_loop(
        1, lax.axis_size(axis), lambda source, state: combine(state, take(source)), take(0)
    )


def repeat_heads(stat):
    return jnp.repeat(stat, HD, axis=-1)


def combine(earlier, later):
    best = jnp.maximum(earlier[0], later[0])
    factor_one = jnp.exp(earlier[0] - best)
    factor_two = jnp.exp(later[0] - best)
    denom = earlier[1] * factor_one + later[1] * factor_two
    summed = earlier[2] * repeat_heads(factor_one) + later[2] * repeat_heads(factor_two)
    return (best, denom, summed)


def general_body(hist_keys, hist_values, latent_queries, latent_pos, targets, out_proj, norm_gain, unembed):
    softmax_scale = HD ** (-0.5)
    seq_keys = hist_keys[0]
    seq_values = hist_values[0]
    position = lax.axis_index("seq")
    tok_rows = seq_keys.shape[0]
    channels = seq_keys.shape[1]
    head_count = channels // HD
    own_rows = latent_queries.shape[1]
    queries = lax.all_gather(latent_queries[0], "seq", axis=0, tiled=True)
    latents = queries.shape[0]
    query_heads = queries.reshape(latents, head_count, HD)
    key_heads = seq_keys.reshape(tok_rows, head_count, HD)
    value_heads = seq_values.reshape(tok_rows, head_count, HD)
    places = position * tok_rows + jnp.arange(tok_rows, dtype=jnp.int32)
    visible = (places[None, :] <= latent_pos[0][:, None])[None]
    scores = (
        jnp.einsum("ihd,jhd->hij", query_heads, key_heads, preferred_element_type=jnp.float32)
        * softmax_scale
    )
    largest = jnp.max(jnp.where(visible, scores, -1e30), axis=-1)
    weights = jnp.where(visible, jnp.exp(scores - largest[..., None]), 0.0)
    summed = jnp.sum(weights, axis=-1)
    partial_out = jnp.einsum(
        "hij,jhd->ihd",
        weights.astype(jnp.bfloat16),
        value_heads,
        preferred_element_type=jnp.float32,
    ).reshape(latents, channels)
    best, denom, combined = joined((largest.T, summed.T, partial_out), "seq", combine)
    attn_all = (combined / repeat_heads(denom)).astype(jnp.bfloat16)
    log_norm = best + jnp.log(denom)
    slab = out_proj.shape[0]
    attn_cols = lax.dynamic_slice_in_dim(attn_all, position * slab, slab, 1)
    proj_columns = lax.all_to_all(out_proj, "seq", split_axis=1, concat_axis=0, tiled=True)
    column_block = jnp.dot(attn_all, proj_columns, preferred_element_type=jnp.float32)
    hidden = lax.all_to_all(column_block, "seq", split_axis=0, concat_axis=1, tiled=True)
    inverse = lax.rsqrt(jnp.mean(hidden * hidden, axis=-1, keepdims=True) + epsilon)
    normed = (hidden * inverse * norm_gain).astype(jnp.bfloat16)
    logits = jnp.dot(normed, unembed, preferred_element_type=jnp.float32)
    log_total = jax.nn.logsumexp(logits, axis=-1, keepdims=True)
    onehot = (jnp.arange(logits.shape[1], dtype=jnp.int32)[None, :] == targets[0][:, None]).astype(
        jnp.float32
    )
    local_loss = jnp.sum(log_total[:, 0] - jnp.sum(logits * onehot, axis=-1))
    grad_logits = (loss_factor * (jnp.exp(logits - log_total) - onehot)).astype(jnp.bfloat16)
    grad_normed = lax.dot_general(
        grad_logits, unembed, (((1,), (1,)), ((), ())), preferred_element_type=jnp.float32
    )
    scaled = norm_gain * grad_normed
    grad_hidden = (
        inverse * scaled - hidden * inverse**3 * jnp.mean(hidden * scaled, axis=-1, keepdims=True)
    ).astype(jnp.bfloat16)
    grad_all = lax.all_gather(grad_hidden, "seq", axis=0, tiled=True)
    weight_part = lax.dot_general(
        attn_cols, grad_all, (((0,), (0,)), ((), ())), preferred_element_type=jnp.float32
    )
    grad_cols = lax.dot_general(
        grad_all, out_proj, (((1,), (1,)), ((), ())), preferred_element_type=jnp.float32
    ).astype(jnp.bfloat16)
    grad_attn = lax.all_gather(grad_cols, "seq", axis=1, tiled=True)
    grad_heads = grad_attn.reshape(latents, head_count, HD)
    product = grad_attn.astype(jnp.float32) * attn_all.astype(jnp.float32)
    delta = jnp.sum(product.reshape(latents, head_count, HD), axis=-1)
    probs = jnp.where(visible, jnp.exp(scores - log_norm.T[..., None]), 0.0)
    grad_probs = jnp.einsum(
        "ihd,jhd->hij", grad_heads, value_heads, preferred_element_type=jnp.float32
    )
    grad_scores = (probs * (grad_probs - delta.T[..., None])).astype(jnp.bfloat16)
    grad_values = (
        jnp.einsum(
            "hij,ihd->jhd",
            probs.astype(jnp.bfloat16),
            grad_heads,
            preferred_element_type=jnp.float32,
        )
        .reshape(tok_rows, channels)
        .astype(jnp.bfloat16)
    )
    grad_keys = (
        (
            jnp.einsum("hij,ihd->jhd", grad_scores, query_heads, preferred_element_type=jnp.float32)
            * softmax_scale
        )
        .reshape(tok_rows, channels)
        .astype(jnp.bfloat16)
    )
    terms = jnp.einsum("hij,jhd->ihd", grad_scores, key_heads, preferred_element_type=jnp.float32)
    grad_queries = lax.psum_scatter(
        (terms.reshape(lax.axis_size("seq") * own_rows, channels) * softmax_scale).astype(
            jnp.bfloat16
        ),
        "seq",
        scatter_dimension=0,
        tiled=True,
    )
    entries = channels * D
    weight_sum = lax.psum(weight_part.astype(jnp.bfloat16), "grp").astype(jnp.float32)
    loss_sum, square_sum = lax.psum((local_loss, jnp.sum(weight_sum * weight_sum)), "seq")
    proj_update = weight_sum * lax.rsqrt(square_sum / entries + epsilon)
    return (
        loss_sum.reshape(1),
        grad_queries[None],
        grad_keys[None],
        grad_values[None],
        proj_update,
    )


VMEM = pl.BlockSpec(memory_space=pltpu.VMEM)
SMEM = pl.BlockSpec(memory_space=pltpu.SMEM)
VMEM_LIMIT = 16 << 20
ROWS_T = (((1,), (1,)), ((), ()))
COLS_T = (((0,), (0,)), ((), ()))


def matmul(one, two, dims=(((1,), (0,)), ((), ()))):
    return lax.dot_general(one, two, dims, preferred_element_type=jnp.float32)


def kernel_call(kernel, in_specs, outs, scratch=(), flops=1 << 20, on_chip=True):
    shaped = pltpu.VMEM if on_chip else jax.ShapeDtypeStruct
    call = pl.pallas_call(
        kernel,
        in_specs=in_specs,
        out_specs=[VMEM] * len(outs),
        out_shape=[shaped(shape, dtype) for shape, dtype in outs],
        scratch_shapes=list(scratch),
        cost_estimate=pl.CostEstimate(flops=flops, bytes_accessed=0, transcendentals=0),
        compiler_params=pltpu.CompilerParams(vmem_limit_bytes=VMEM_LIMIT),
    )

    def placed(*operands):
        return call(
            *(
                pltpu.with_memory_space_constraint(operand, pltpu.VMEM) if spec is VMEM else operand
                for spec, operand in zip(in_specs, operands)
            )
        )

    return placed


def pack_kernel(targets, keys, values, queries, packed):
    heads = packed.shape[0]
    tok = keys.shape[0]
    own = queries.shape[0]
    lanes = lax.broadcasted_iota(jnp.int32, (own, HD), 1)
    rows = lax.broadcasted_iota(jnp.int32, (own, HD), 0)
    wanted = jnp.zeros((own, HD), jnp.int32)
    for row in range(own):
        wanted = jnp.where(rows == row, targets[0, row], wanted)
    onehot = (lanes == wanted).astype(jnp.float32)
    for head in range(heads):
        cols = slice(head * HD, (head + 1) * HD)
        packed[head, 0:tok, :] = keys[:, cols]
        packed[head, tok : 2 * tok, :] = values[:, cols]
        tail = jnp.concatenate([queries[:, cols].astype(jnp.float32), onehot], axis=0)
        packed[head, 2 * tok : 2 * tok + 2 * own, :] = tail.astype(jnp.bfloat16)


def split_packed(packed, tok, own):
    heads = packed.shape[0]
    keys = packed[:, 0:tok, :].reshape(heads * tok, HD)
    values = packed[:, tok : 2 * tok, :].reshape(heads * tok, HD)
    queries = packed[:, 2 * tok : 2 * tok + own, :].astype(jnp.float32).reshape(heads * own, HD)
    return keys, values, queries.astype(jnp.bfloat16)


def visible_scores(keys, queries, positions):
    latents = queries.shape[0]
    length = keys.shape[0]
    diagonal = lax.broadcasted_iota(jnp.int32, (latents, latents), 0) == lax.broadcasted_iota(
        jnp.int32, (latents, latents), 1
    )
    last = jnp.sum(
        jnp.where(diagonal, positions[...].astype(jnp.float32), 0.0), axis=1, keepdims=True
    )
    places = lax.broadcasted_iota(jnp.int32, (latents, length), 1).astype(jnp.float32)
    scores = matmul(queries, keys, ROWS_T) * HD ** (-0.5)
    return scores, places <= last


def forward_kernel(side, positions, packed, out_proj, attn, log_norm, onehot, kept, sent, hidden, *, tok, own):
    keys, values, queries = split_packed(packed, tok, own)
    scores, visible = visible_scores(keys, queries, positions)
    best = jnp.max(jnp.where(visible, scores, -1e30), axis=-1, keepdims=True)
    weights = jnp.where(visible, jnp.exp(scores - best), 0.0)
    denom = jnp.sum(weights, axis=-1, keepdims=True)
    summed = matmul(weights.astype(jnp.bfloat16), values)
    attn[...] = (summed / denom).astype(jnp.bfloat16)
    log_norm[...] = jnp.broadcast_to(best + jnp.log(denom), log_norm.shape)
    half = kept.shape[0]
    mine = side[0]
    pieces = half // own
    onehot[...] = (
        packed[pl.ds(mine * pieces, pieces), 2 * tok + own : 2 * tok + 2 * own, :]
        .astype(jnp.float32)
        .reshape(half, HD)
    )
    hidden[...] = matmul(attn[...], out_proj[...])
    kept[...] = hidden[pl.ds(pl.multiple_of(mine * half, half), half), :]
    sent[...] = hidden[pl.ds(pl.multiple_of((1 - mine) * half, half), half), :].astype(sent.dtype)


def loss_kernel(gain, unembed, onehot_ref, attn, *refs):
    *parts, message, stats = refs
    half = onehot_ref.shape[0]
    hidden = parts[0][...].astype(jnp.float32)
    for part in parts[1:]:
        hidden = hidden + part[...].astype(jnp.float32)
    onehot = onehot_ref[...]
    inverse = lax.rsqrt(jnp.mean(hidden * hidden, axis=-1, keepdims=True) + epsilon)
    normed = (hidden * inverse * gain[...]).astype(jnp.bfloat16)
    logits = matmul(normed, unembed[...])
    top = jnp.max(logits, axis=-1, keepdims=True)
    log_total = top + jnp.log(jnp.sum(jnp.exp(logits - top), axis=-1, keepdims=True))
    losses = log_total - jnp.sum(logits * onehot, axis=-1, keepdims=True)
    stats[...] = jnp.broadcast_to(jnp.sum(losses, axis=0, keepdims=True), stats.shape)
    grad_logits = (loss_factor * (jnp.exp(logits - log_total) - onehot)).astype(jnp.bfloat16)
    scaled = gain[...] * matmul(grad_logits, unembed[...], ROWS_T)
    mean = jnp.mean(hidden * scaled, axis=-1, keepdims=True)
    grad_hidden = (inverse * scaled - hidden * (inverse * inverse * inverse) * mean).astype(
        jnp.bfloat16
    )
    blocks = hidden.shape[1] // HD
    for block in range(blocks):
        message[block * half : (block + 1) * half, :] = grad_hidden[:, block * HD : (block + 1) * HD]
    message[blocks * half :, :] = attn[...]


def fill_rows(target, row, message, half):
    for block in range(target.shape[1] // HD):
        target[pl.ds(row, half), block * HD : (block + 1) * HD] = message[
            block * half : (block + 1) * half, :
        ]


def backward_kernel(
    side, positions, packed, out_proj, attn, log_norm, own_msg, pair_msg, grads, grad_hidden, *, tok, own
):
    half = grad_hidden.shape[0] // 2
    mine = side[0]
    fill_rows(grad_hidden, pl.multiple_of(mine * half, half), own_msg, half)
    fill_rows(grad_hidden, pl.multiple_of((1 - mine) * half, half), pair_msg, half)
    keys, values, queries = split_packed(packed, tok, own)
    scores, visible = visible_scores(keys, queries, positions)
    heads = packed.shape[0]
    grad_attn = matmul(grad_hidden[...], out_proj[...], ROWS_T).astype(jnp.bfloat16)
    delta = jnp.sum(
        grad_attn.astype(jnp.float32) * attn[...].astype(jnp.float32), axis=-1, keepdims=True
    )
    probs = jnp.where(visible, jnp.exp(scores - log_norm[:, 0:1]), 0.0)
    grad_probs = matmul(grad_attn, values, ROWS_T)
    grad_scores = (probs * (grad_probs - delta)).astype(jnp.bfloat16)
    grad_values = matmul(probs.astype(jnp.bfloat16), grad_attn, COLS_T).astype(jnp.bfloat16)
    scale = HD ** (-0.5)
    grad_keys = (matmul(grad_scores, queries, COLS_T) * scale).astype(jnp.bfloat16)
    grad_queries = matmul(grad_scores, keys) * scale
    grads[:, 0:tok, :] = grad_keys.reshape(heads, tok, HD)
    grads[:, tok : 2 * tok, :] = grad_values.reshape(heads, tok, HD)
    tail = grad_queries.reshape(heads, own, HD)
    grads[:, 2 * tok : 2 * tok + 2 * own, :] = jnp.concatenate([tail, tail], axis=1).astype(
        jnp.bfloat16
    )


def unpack_kernel(packed, grad_queries, grad_keys, grad_values):
    heads = packed.shape[0]
    tok = grad_keys.shape[0]
    own = grad_queries.shape[0]
    for head in range(heads):
        cols = slice(head * HD, (head + 1) * HD)
        grad_keys[:, cols] = packed[head, 0:tok, :]
        grad_values[:, cols] = packed[head, tok : 2 * tok, :]
        grad_queries[:, cols] = packed[head, 2 * tok : 2 * tok + own, :]


def weight_kernel(side, *refs, count):
    messages = refs[: 2 * count]
    loss, weights, stats, attn_rows, grad_rows = refs[2 * count :]
    half = grad_rows.shape[0] // (2 * count)
    blocks = grad_rows.shape[1] // HD
    mine = side[0]
    for index in range(count):
        attn_at = blocks * half
        for place, message, part in (
            (0, messages[index], mine),
            (1, messages[count + index], 1 - mine),
        ):
            row = (2 * index + place) * half
            for block in range(blocks):
                grad_rows[row : row + half, block * HD : (block + 1) * HD] = message[
                    block * half : (block + 1) * half, :
                ]
            attn_rows[row : row + half, :] = messages[index][
                pl.ds(pl.multiple_of(attn_at + part * half, half), half), :
            ]
    total = matmul(attn_rows[...], grad_rows[...], COLS_T)
    weights[...] = total
    squares = jnp.sum(jnp.sum(total * total, axis=0, keepdims=True), axis=1, keepdims=True)
    lanes = lax.broadcasted_iota(jnp.int32, stats.shape, 1)
    stats[...] = jnp.where(lanes < HD // 2, squares, loss[...])


def body(hist_keys, hist_values, latent_queries, latent_pos, targets, out_proj, norm_gain, unembed):
    n_seq = lax.axis_size("seq")
    n_grp = lax.axis_size("grp")
    seq_keys = hist_keys[0]
    tok, channels = seq_keys.shape
    own = latent_queries.shape[1]
    latents = n_seq * own
    heads = channels // HD
    vocab = unembed.shape[1]
    if not (
        heads == n_seq
        and out_proj.shape[0] == HD
        and vocab == HD
        and tok % 16 == 0
        and own == 8
        and n_seq & (n_seq - 1) == 0
        and n_seq > 1
    ):
        return general_body(
            hist_keys, hist_values, latent_queries, latent_pos, targets, out_proj, norm_gain, unembed
        )
    bf16, f32 = jnp.bfloat16, jnp.float32
    half = latents // 2
    width = out_proj.shape[1]
    span = 2 * tok + 2 * own
    side = (lax.axis_index("seq") % 2).reshape(1)
    swap = [(i, i ^ 1) for i in range(n_seq)]

    (packed,) = kernel_call(
        pack_kernel, [SMEM, VMEM, VMEM, VMEM], [((heads, span, HD), bf16)]
    )(targets, seq_keys, hist_values[0], latent_queries[0])
    packed = lax.all_to_all(packed, "seq", 0, 0)

    attn, log_norm, onehot, kept, sent = kernel_call(
        partial(forward_kernel, tok=tok, own=own),
        [SMEM, VMEM, VMEM, VMEM],
        [
            ((latents, HD), bf16),
            ((latents, HD), f32),
            ((half, HD), f32),
            ((half, width), f32),
            ((half, width), bf16),
        ],
        [pltpu.VMEM((latents, width), f32)],
    )(side, latent_pos, packed, out_proj)
    pair_sum = (kept + lax.ppermute(sent, "seq", swap).astype(f32)).astype(bf16)
    parts = [pair_sum] + [
        lax.ppermute(pair_sum, "seq", [(i, i ^ step) for i in range(n_seq)])
        for step in range(2, n_seq, 2)
    ]
    message, loss = kernel_call(
        loss_kernel,
        [VMEM] * (4 + len(parts)),
        [((width // HD * half + latents, HD), bf16), ((1, HD), f32)],
    )(norm_gain.reshape(1, width), unembed, onehot, attn, *parts)
    pair_msg = lax.ppermute(message, "seq", swap)
    others = [
        lax.ppermute(message, "grp", [(i, (i + step) % n_grp) for i in range(n_grp)])
        for step in range(1, n_grp)
    ]
    backward = kernel_call(
        partial(backward_kernel, tok=tok, own=own),
        [SMEM] + [VMEM] * 7,
        [((heads, span, HD), bf16)],
        [pltpu.VMEM((latents, width), bf16)],
        flops=1 << 30,
    )
    (grads,) = backward(side, latent_pos, packed, out_proj, attn, log_norm, message, pair_msg)
    others = lax.optimization_barrier((*others, grads))[:-1]
    grads = lax.all_to_all(grads, "seq", 0, 0)
    pair_others = [lax.ppermute(other, "seq", swap) for other in others]
    weights, stats = kernel_call(
        partial(weight_kernel, count=n_grp),
        [SMEM] + [VMEM] * (2 * n_grp + 1),
        [((channels // n_seq, width), f32), ((1, HD), f32)],
        [
            pltpu.VMEM((n_grp * latents, HD), bf16),
            pltpu.VMEM((n_grp * latents, width), bf16),
        ],
    )(side, message, *others, pair_msg, *pair_others, loss)
    grad_queries, grad_keys, grad_values = kernel_call(
        unpack_kernel,
        [VMEM],
        [((own, channels), bf16), ((tok, channels), bf16), ((tok, channels), bf16)],
        on_chip=False,
    )(grads)
    stats = stats + lax.ppermute(stats, "seq", swap)
    received = [
        lax.ppermute(stats, "seq", [(i, i ^ step) for i in range(n_seq)])
        for step in range(2, n_seq, 2)
    ]
    received = lax.optimization_barrier((*received, grad_queries))[:-1]
    totals = sum(received, stats)[0]
    loss_sum = totals[HD - 1] / (n_seq // 2)
    proj_update = weights * lax.rsqrt(totals[0] / (channels * width) + epsilon)
    return (
        loss_sum.reshape(1),
        grad_queries[None],
        grad_keys[None],
        grad_values[None],
        proj_update,
    )


def solution(mesh):
    placed = (
        P("grp", "seq", None),
        P("grp", "seq", None),
        P("grp", "seq", None),
        P("grp", None),
        P("grp", "seq"),
        P("seq", None),
        P(),
        P(),
    )
    return jax.shard_map(
        body,
        mesh=mesh,
        in_specs=placed,
        out_specs=(
            P("grp"),
            P("grp", "seq", None),
            P("grp", "seq", None),
            P("grp", "seq", None),
            P("seq", None),
        ),
        check_vma=False,
    )
```

```python
from functools import partial

import jax
import jax.numpy as jnp
from jax import lax
from jax.experimental import pallas as pl
from jax.experimental.pallas import tpu as pltpu
from jax.sharding import PartitionSpec as P


D = 2048
HD = 128


epsilon = 1e-06
loss_factor = 64.0


def joined(part, axis, combine):
    gathered = jax.tree.map(lambda a: lax.all_gather(a, axis), part)

    def take(source):
        return jax.tree.map(lambda a: lax.dynamic_index_in_dim(a, source, 0, False), gathered)

    return lax.fori_loop(
        1, lax.axis_size(axis), lambda source, state: combine(state, take(source)), take(0)
    )


def repeat_heads(stat):
    return jnp.repeat(stat, HD, axis=-1)


def combine(earlier, later):
    best = jnp.maximum(earlier[0], later[0])
    factor_one = jnp.exp(earlier[0] - best)
    factor_two = jnp.exp(later[0] - best)
    denom = earlier[1] * factor_one + later[1] * factor_two
    summed = earlier[2] * repeat_heads(factor_one) + later[2] * repeat_heads(factor_two)
    return (best, denom, summed)


def general_body(hist_keys, hist_values, latent_queries, latent_pos, targets, out_proj, norm_gain, unembed):
    softmax_scale = HD ** (-0.5)
    seq_keys = hist_keys[0]
    seq_values = hist_values[0]
    position = lax.axis_index("seq")
    tok_rows = seq_keys.shape[0]
    channels = seq_keys.shape[1]
    head_count = channels // HD
    own_rows = latent_queries.shape[1]
    queries = lax.all_gather(latent_queries[0], "seq", axis=0, tiled=True)
    latents = queries.shape[0]
    query_heads = queries.reshape(latents, head_count, HD)
    key_heads = seq_keys.reshape(tok_rows, head_count, HD)
    value_heads = seq_values.reshape(tok_rows, head_count, HD)
    places = position * tok_rows + jnp.arange(tok_rows, dtype=jnp.int32)
    visible = (places[None, :] <= latent_pos[0][:, None])[None]
    scores = (
        jnp.einsum("ihd,jhd->hij", query_heads, key_heads, preferred_element_type=jnp.float32)
        * softmax_scale
    )
    largest = jnp.max(jnp.where(visible, scores, -1e30), axis=-1)
    weights = jnp.where(visible, jnp.exp(scores - largest[..., None]), 0.0)
    summed = jnp.sum(weights, axis=-1)
    partial_out = jnp.einsum(
        "hij,jhd->ihd",
        weights.astype(jnp.bfloat16),
        value_heads,
        preferred_element_type=jnp.float32,
    ).reshape(latents, channels)
    best, denom, combined = joined((largest.T, summed.T, partial_out), "seq", combine)
    attn_all = (combined / repeat_heads(denom)).astype(jnp.bfloat16)
    log_norm = best + jnp.log(denom)
    slab = out_proj.shape[0]
    attn_cols = lax.dynamic_slice_in_dim(attn_all, position * slab, slab, 1)
    proj_columns = lax.all_to_all(out_proj, "seq", split_axis=1, concat_axis=0, tiled=True)
    column_block = jnp.dot(attn_all, proj_columns, preferred_element_type=jnp.float32)
    hidden = lax.all_to_all(column_block, "seq", split_axis=0, concat_axis=1, tiled=True)
    inverse = lax.rsqrt(jnp.mean(hidden * hidden, axis=-1, keepdims=True) + epsilon)
    normed = (hidden * inverse * norm_gain).astype(jnp.bfloat16)
    logits = jnp.dot(normed, unembed, preferred_element_type=jnp.float32)
    log_total = jax.nn.logsumexp(logits, axis=-1, keepdims=True)
    onehot = (jnp.arange(logits.shape[1], dtype=jnp.int32)[None, :] == targets[0][:, None]).astype(
        jnp.float32
    )
    local_loss = jnp.sum(log_total[:, 0] - jnp.sum(logits * onehot, axis=-1))
    grad_logits = (loss_factor * (jnp.exp(logits - log_total) - onehot)).astype(jnp.bfloat16)
    grad_normed = lax.dot_general(
        grad_logits, unembed, (((1,), (1,)), ((), ())), preferred_element_type=jnp.float32
    )
    scaled = norm_gain * grad_normed
    grad_hidden = (
        inverse * scaled - hidden * inverse**3 * jnp.mean(hidden * scaled, axis=-1, keepdims=True)
    ).astype(jnp.bfloat16)
    grad_all = lax.all_gather(grad_hidden, "seq", axis=0, tiled=True)
    weight_part = lax.dot_general(
        attn_cols, grad_all, (((0,), (0,)), ((), ())), preferred_element_type=jnp.float32
    )
    grad_cols = lax.dot_general(
        grad_all, out_proj, (((1,), (1,)), ((), ())), preferred_element_type=jnp.float32
    ).astype(jnp.bfloat16)
    grad_attn = lax.all_gather(grad_cols, "seq", axis=1, tiled=True)
    grad_heads = grad_attn.reshape(latents, head_count, HD)
    product = grad_attn.astype(jnp.float32) * attn_all.astype(jnp.float32)
    delta = jnp.sum(product.reshape(latents, head_count, HD), axis=-1)
    probs = jnp.where(visible, jnp.exp(scores - log_norm.T[..., None]), 0.0)
    grad_probs = jnp.einsum(
        "ihd,jhd->hij", grad_heads, value_heads, preferred_element_type=jnp.float32
    )
    grad_scores = (probs * (grad_probs - delta.T[..., None])).astype(jnp.bfloat16)
    grad_values = (
        jnp.einsum(
            "hij,ihd->jhd",
            probs.astype(jnp.bfloat16),
            grad_heads,
            preferred_element_type=jnp.float32,
        )
        .reshape(tok_rows, channels)
        .astype(jnp.bfloat16)
    )
    grad_keys = (
        (
            jnp.einsum("hij,ihd->jhd", grad_scores, query_heads, preferred_element_type=jnp.float32)
            * softmax_scale
        )
        .reshape(tok_rows, channels)
        .astype(jnp.bfloat16)
    )
    terms = jnp.einsum("hij,jhd->ihd", grad_scores, key_heads, preferred_element_type=jnp.float32)
    grad_queries = lax.psum_scatter(
        (terms.reshape(lax.axis_size("seq") * own_rows, channels) * softmax_scale).astype(
            jnp.bfloat16
        ),
        "seq",
        scatter_dimension=0,
        tiled=True,
    )
    entries = channels * D
    weight_sum = lax.psum(weight_part.astype(jnp.bfloat16), "grp").astype(jnp.float32)
    loss_sum, square_sum = lax.psum((local_loss, jnp.sum(weight_sum * weight_sum)), "seq")
    proj_update = weight_sum * lax.rsqrt(square_sum / entries + epsilon)
    return (
        loss_sum.reshape(1),
        grad_queries[None],
        grad_keys[None],
        grad_values[None],
        proj_update,
    )


VMEM = pl.BlockSpec(memory_space=pltpu.VMEM)
SMEM = pl.BlockSpec(memory_space=pltpu.SMEM)
KEPT = object()
LOSS_ROWS = 16
VMEM_LIMIT = 16 << 20
ROWS_T = (((1,), (1,)), ((), ()))
COLS_T = (((0,), (0,)), ((), ()))


def matmul(one, two, dims=(((1,), (0,)), ((), ()))):
    return lax.dot_general(one, two, dims, preferred_element_type=jnp.float32)


def kernel_call(kernel, in_specs, outs, scratch=(), flops=1 << 20, held=pltpu.VMEM):
    call = pl.pallas_call(
        kernel,
        in_specs=in_specs,
        out_specs=[VMEM if spec is KEPT else spec for _, _, spec in outs],
        out_shape=[
            (pltpu.VMEM if spec is KEPT else jax.ShapeDtypeStruct)(shape, dtype)
            for shape, dtype, spec in outs
        ],
        scratch_shapes=list(scratch),
        cost_estimate=pl.CostEstimate(flops=flops, bytes_accessed=0, transcendentals=0),
        compiler_params=pltpu.CompilerParams(vmem_limit_bytes=VMEM_LIMIT),
    )

    def placed(*operands):
        return call(
            *(
                pltpu.with_memory_space_constraint(operand, held)
                if spec is VMEM or held is pltpu.HBM
                else operand
                for spec, operand in zip(in_specs, operands)
            )
        )

    return placed


def pack_kernel(targets, keys, values, queries, packed):
    heads = packed.shape[0]
    tok = keys.shape[0]
    own = queries.shape[0]
    lanes = lax.broadcasted_iota(jnp.int32, (own, HD), 1)
    rows = lax.broadcasted_iota(jnp.int32, (own, HD), 0)
    wanted = jnp.zeros((own, HD), jnp.int32)
    for row in range(own):
        wanted = jnp.where(rows == row, targets[0, row], wanted)
    onehot = (lanes == wanted).astype(jnp.float32)
    for head in range(heads):
        cols = slice(head * HD, (head + 1) * HD)
        packed[head, 0:tok, :] = keys[:, cols]
        packed[head, tok : 2 * tok, :] = values[:, cols]
        tail = jnp.concatenate([queries[:, cols].astype(jnp.float32), onehot], axis=0)
        packed[head, 2 * tok : 2 * tok + 2 * own, :] = tail.astype(jnp.bfloat16)


def split_packed(packed, tok, own):
    heads = packed.shape[0]
    keys = packed[:, 0:tok, :].reshape(heads * tok, HD)
    values = packed[:, tok : 2 * tok, :].reshape(heads * tok, HD)
    queries = packed[:, 2 * tok : 2 * tok + own, :].astype(jnp.float32).reshape(heads * own, HD)
    return keys, values, queries.astype(jnp.bfloat16)


def visible_scores(keys, queries, positions):
    latents = queries.shape[0]
    length = keys.shape[0]
    diagonal = lax.broadcasted_iota(jnp.int32, (latents, latents), 0) == lax.broadcasted_iota(
        jnp.int32, (latents, latents), 1
    )
    last = jnp.sum(
        jnp.where(diagonal, positions[...].astype(jnp.float32), 0.0), axis=1, keepdims=True
    )
    places = lax.broadcasted_iota(jnp.int32, (latents, length), 1).astype(jnp.float32)
    scores = matmul(queries, keys, ROWS_T) * HD ** (-0.5)
    return scores, places <= last


def forward_kernel(side, positions, packed, out_proj, attn, log_norm, onehot, kept, sent, hidden, *, tok, own):
    keys, values, queries = split_packed(packed, tok, own)
    scores, visible = visible_scores(keys, queries, positions)
    best = jnp.max(jnp.where(visible, scores, -1e30), axis=-1, keepdims=True)
    weights = jnp.where(visible, jnp.exp(scores - best), 0.0)
    denom = jnp.sum(weights, axis=-1, keepdims=True)
    summed = matmul(weights.astype(jnp.bfloat16), values)
    attn[...] = (summed / denom).astype(jnp.bfloat16)
    log_norm[...] = jnp.broadcast_to(best + jnp.log(denom), log_norm.shape)
    half = kept.shape[0]
    mine = side[0]
    pieces = half // own
    onehot[...] = (
        packed[pl.ds(mine * pieces, pieces), 2 * tok + own : 2 * tok + 2 * own, :]
        .astype(jnp.float32)
        .reshape(half, HD)
    )
    hidden[...] = matmul(attn[...], out_proj[...])
    kept[...] = hidden[pl.ds(pl.multiple_of(mine * half, half), half), :]
    sent[...] = hidden[pl.ds(pl.multiple_of((1 - mine) * half, half), half), :].astype(sent.dtype)


def exact_parts(value):
    high = value.astype(jnp.bfloat16).astype(jnp.float32)
    middle = (value - high).astype(jnp.bfloat16).astype(jnp.float32)
    return high, middle, value - high - middle


def loss_kernel(gain, unembed, onehot_ref, *refs):
    *parts, message, stats = refs
    half = onehot_ref.shape[0]
    hidden = parts[0][...].astype(jnp.float32)
    for part in parts[1:]:
        hidden = hidden + part[...].astype(jnp.float32)
    onehot = onehot_ref[...]
    inverse = lax.rsqrt(jnp.mean(hidden * hidden, axis=-1, keepdims=True) + epsilon)
    normed = (hidden * inverse * gain[...]).astype(jnp.bfloat16)
    logits = matmul(normed, unembed[...])
    top = jnp.max(logits, axis=-1, keepdims=True)
    log_total = top + jnp.log(jnp.sum(jnp.exp(logits - top), axis=-1, keepdims=True))
    losses = log_total - jnp.sum(logits * onehot, axis=-1, keepdims=True)
    total = jnp.broadcast_to(jnp.sum(losses, axis=0, keepdims=True), stats.shape)
    stats[...] = total
    grad_logits = (loss_factor * (jnp.exp(logits - log_total) - onehot)).astype(jnp.bfloat16)
    scaled = gain[...] * matmul(grad_logits, unembed[...], ROWS_T)
    mean = jnp.mean(hidden * scaled, axis=-1, keepdims=True)
    grad_hidden = (inverse * scaled - hidden * (inverse * inverse * inverse) * mean).astype(
        jnp.bfloat16
    )
    blocks = hidden.shape[1] // HD
    for block in range(blocks):
        message[block * half : (block + 1) * half, :] = grad_hidden[:, block * HD : (block + 1) * HD]
    row = lax.broadcasted_iota(jnp.int32, (LOSS_ROWS, HD), 0)
    high, middle, low = exact_parts(total)
    message[blocks * half :, :] = jnp.where(
        row == 0, high, jnp.where(row == 1, middle, jnp.where(row == 2, low, 0.0))
    ).astype(jnp.bfloat16)


def fill_rows(target, row, message, half):
    for block in range(target.shape[1] // HD):
        target[pl.ds(row, half), block * HD : (block + 1) * HD] = message[
            block * half : (block + 1) * half, :
        ]


def backward_kernel(
    side,
    positions,
    packed,
    out_proj,
    attn,
    log_norm,
    own_msg,
    pair_msg,
    grads,
    grad_hidden,
    *,
    tok,
    own,
):
    half = grad_hidden.shape[0] // 2
    mine = side[0]
    fill_rows(grad_hidden, pl.multiple_of(mine * half, half), own_msg, half)
    fill_rows(grad_hidden, pl.multiple_of((1 - mine) * half, half), pair_msg, half)
    keys, values, queries = split_packed(packed, tok, own)
    scores, visible = visible_scores(keys, queries, positions)
    heads = packed.shape[0]
    grad_attn = matmul(grad_hidden[...], out_proj[...], ROWS_T).astype(jnp.bfloat16)
    delta = jnp.sum(
        grad_attn.astype(jnp.float32) * attn[...].astype(jnp.float32), axis=-1, keepdims=True
    )
    probs = jnp.where(visible, jnp.exp(scores - log_norm[:, 0:1]), 0.0)
    grad_probs = matmul(grad_attn, values, ROWS_T)
    grad_scores = (probs * (grad_probs - delta)).astype(jnp.bfloat16)
    grad_values = matmul(probs.astype(jnp.bfloat16), grad_attn, COLS_T).astype(jnp.bfloat16)
    scale = HD ** (-0.5)
    grad_keys = (matmul(grad_scores, queries, COLS_T) * scale).astype(jnp.bfloat16)
    grad_queries = matmul(grad_scores, keys) * scale
    grads[:, 0:tok, :] = grad_keys.reshape(heads, tok, HD)
    grads[:, tok : 2 * tok, :] = grad_values.reshape(heads, tok, HD)
    tail = grad_queries.reshape(heads, own, HD)
    grads[:, 2 * tok : 2 * tok + 2 * own, :] = jnp.concatenate([tail, tail], axis=1).astype(
        jnp.bfloat16
    )


def unpack_kernel(packed, grad_queries, grad_keys, grad_values):
    heads = packed.shape[0]
    tok = grad_keys.shape[0]
    own = grad_queries.shape[0]
    for head in range(heads):
        cols = slice(head * HD, (head + 1) * HD)
        grad_keys[:, cols] = packed[head, 0:tok, :]
        grad_values[:, cols] = packed[head, tok : 2 * tok, :]
        grad_queries[:, cols] = packed[head, 2 * tok : 2 * tok + own, :]


def weight_kernel(side, *refs, groups, seqs, entries):
    own_msgs = refs[:groups]
    pair_msgs = refs[groups : 2 * groups]
    attns = refs[2 * groups : 2 * groups + seqs]
    loss_half, update, loss, grad_hidden, total = refs[2 * groups + seqs :]
    latents = grad_hidden.shape[0] // groups
    half = latents // 2
    mine = side[0]
    for index in range(groups):
        first = index * latents
        fill_rows(
            grad_hidden, pl.multiple_of(first + mine * half, half), own_msgs[index], half
        )
        fill_rows(
            grad_hidden, pl.multiple_of(first + (1 - mine) * half, half), pair_msgs[index], half
        )
    squares = jnp.zeros((8, total.shape[1]), jnp.float32)
    for index in range(seqs):
        part = matmul(attns[index][...], grad_hidden[...], COLS_T)
        if index == 0:
            total[...] = part
        squares = squares + jnp.sum((part * part).reshape(HD // 8, 8, total.shape[1]), axis=0)
    square_sum = jnp.sum(jnp.sum(squares, axis=0, keepdims=True), axis=1, keepdims=True)
    update[...] = total[...] * lax.rsqrt(square_sum / entries + epsilon)
    other_loss = jnp.sum(pair_msgs[0][-LOSS_ROWS:, :].astype(jnp.float32), axis=0, keepdims=True)
    loss[...] = loss_half[...] + other_loss


def body(hist_keys, hist_values, latent_queries, latent_pos, targets, out_proj, norm_gain, unembed):
    n_seq = lax.axis_size("seq")
    n_grp = lax.axis_size("grp")
    seq_keys = hist_keys[0]
    tok, channels = seq_keys.shape
    own = latent_queries.shape[1]
    latents = n_seq * own
    heads = channels // HD
    vocab = unembed.shape[1]
    if not (
        heads == n_seq
        and out_proj.shape[0] == HD
        and vocab == HD
        and tok % 16 == 0
        and own == 8
        and n_seq & (n_seq - 1) == 0
        and n_seq > 1
    ):
        return general_body(
            hist_keys, hist_values, latent_queries, latent_pos, targets, out_proj, norm_gain, unembed
        )
    bf16, f32 = jnp.bfloat16, jnp.float32
    half = latents // 2
    width = out_proj.shape[1]
    span = 2 * tok + 2 * own
    side = (lax.axis_index("seq") % 2).reshape(1)
    swap = [(i, i ^ 1) for i in range(n_seq)]

    (packed,) = kernel_call(
        pack_kernel, [SMEM, VMEM, VMEM, VMEM], [((heads, span, HD), bf16, VMEM)], held=pltpu.HBM
    )(targets, seq_keys, hist_values[0], latent_queries[0])
    packed = lax.all_to_all(packed, "seq", 0, 0)

    attn, log_norm, onehot, kept, sent = kernel_call(
        partial(forward_kernel, tok=tok, own=own),
        [SMEM, VMEM, VMEM, VMEM],
        [
            ((latents, HD), bf16, KEPT),
            ((latents, HD), f32, KEPT),
            ((half, HD), f32, KEPT),
            ((half, width), f32, KEPT),
            ((half, width), bf16, KEPT),
        ],
        [pltpu.VMEM((latents, width), f32)],
    )(side, latent_pos, packed, out_proj)
    pair_sum = (kept + lax.ppermute(sent, "seq", swap).astype(f32)).astype(bf16)
    chips = [[(i, i ^ step) for i in range(n_seq)] for step in range(2, n_seq, 2)]
    shifts = [[(i, (i + step) % n_grp) for i in range(n_grp)] for step in range(1, n_grp)]
    parts = [pair_sum] + [lax.ppermute(pair_sum, "seq", perm) for perm in chips]
    attns = [attn] + [lax.ppermute(attn, "grp", perm) for perm in shifts]
    loss_call = kernel_call(
        loss_kernel,
        [VMEM] * (3 + len(parts)),
        [((width // HD * half + LOSS_ROWS, HD), bf16, KEPT), ((1, HD), f32, KEPT)],
        flops=1 << 26,
    )
    message, loss_half = loss_call(norm_gain.reshape(1, width), unembed, onehot, *parts)
    pair_msg = lax.ppermute(message, "seq", swap)
    others = [lax.ppermute(message, "grp", perm) for perm in shifts]
    stack = jnp.concatenate(attns, axis=0)
    stacks = [stack] + [lax.ppermute(stack, "seq", perm) for perm in chips]
    backward = kernel_call(
        partial(backward_kernel, tok=tok, own=own),
        [SMEM] + [VMEM] * 7,
        [((heads, span, HD), bf16, KEPT)],
        [pltpu.VMEM((latents, width), bf16)],
        flops=1 << 30,
    )
    (grads,) = backward(side, latent_pos, packed, out_proj, attn, log_norm, message, pair_msg)
    others = lax.optimization_barrier((*others, grads))[:-1]
    grads = lax.all_to_all(grads, "seq", 0, 0)
    stacks = stacks + [lax.ppermute(one, "seq", swap) for one in stacks]
    pair_others = [lax.ppermute(other, "seq", swap) for other in others]
    proj_update, loss = kernel_call(
        partial(weight_kernel, groups=n_grp, seqs=n_seq, entries=channels * width),
        [SMEM] + [VMEM] * (2 * n_grp + n_seq + 1),
        [((HD, width), f32, VMEM), ((1, HD), f32, VMEM)],
        [
            pltpu.VMEM((n_grp * latents, width), bf16),
            pltpu.VMEM((HD, width), f32),
        ],
    )(side, message, *others, pair_msg, *pair_others, *stacks, loss_half)
    grad_queries, grad_keys, grad_values = kernel_call(
        unpack_kernel,
        [VMEM],
        [
            ((own, channels), bf16, VMEM),
            ((tok, channels), bf16, VMEM),
            ((tok, channels), bf16, VMEM),
        ],
    )(grads)
    loss_sum = loss[0, 0]
    return (
        loss_sum.reshape(1),
        grad_queries[None],
        grad_keys[None],
        grad_values[None],
        proj_update,
    )


def solution(mesh):
    placed = (
        P("grp", "seq", None),
        P("grp", "seq", None),
        P("grp", "seq", None),
        P("grp", None),
        P("grp", "seq"),
        P("seq", None),
        P(),
        P(),
    )
    return jax.shard_map(
        body,
        mesh=mesh,
        in_specs=placed,
        out_specs=(
            P("grp"),
            P("grp", "seq", None),
            P("grp", "seq", None),
            P("grp", "seq", None),
            P("seq", None),
        ),
        check_vma=False,
    )
```

```python
from functools import partial

import jax
import jax.numpy as jnp
from jax import lax
from jax.experimental import pallas as pl
from jax.experimental.pallas import tpu as pltpu
from jax.sharding import PartitionSpec as P


D = 2048
HD = 128


epsilon = 1e-06
loss_factor = 64.0


def joined(part, axis, combine):
    gathered = jax.tree.map(lambda a: lax.all_gather(a, axis), part)

    def take(source):
        return jax.tree.map(lambda a: lax.dynamic_index_in_dim(a, source, 0, False), gathered)

    return lax.fori_loop(
        1, lax.axis_size(axis), lambda source, state: combine(state, take(source)), take(0)
    )


def repeat_heads(stat):
    return jnp.repeat(stat, HD, axis=-1)


def combine(earlier, later):
    best = jnp.maximum(earlier[0], later[0])
    factor_one = jnp.exp(earlier[0] - best)
    factor_two = jnp.exp(later[0] - best)
    denom = earlier[1] * factor_one + later[1] * factor_two
    summed = earlier[2] * repeat_heads(factor_one) + later[2] * repeat_heads(factor_two)
    return (best, denom, summed)


def general_body(hist_keys, hist_values, latent_queries, latent_pos, targets, out_proj, norm_gain, unembed):
    softmax_scale = HD ** (-0.5)
    seq_keys = hist_keys[0]
    seq_values = hist_values[0]
    position = lax.axis_index("seq")
    tok_rows = seq_keys.shape[0]
    channels = seq_keys.shape[1]
    head_count = channels // HD
    own_rows = latent_queries.shape[1]
    queries = lax.all_gather(latent_queries[0], "seq", axis=0, tiled=True)
    latents = queries.shape[0]
    query_heads = queries.reshape(latents, head_count, HD)
    key_heads = seq_keys.reshape(tok_rows, head_count, HD)
    value_heads = seq_values.reshape(tok_rows, head_count, HD)
    places = position * tok_rows + jnp.arange(tok_rows, dtype=jnp.int32)
    visible = (places[None, :] <= latent_pos[0][:, None])[None]
    scores = (
        jnp.einsum("ihd,jhd->hij", query_heads, key_heads, preferred_element_type=jnp.float32)
        * softmax_scale
    )
    largest = jnp.max(jnp.where(visible, scores, -1e30), axis=-1)
    weights = jnp.where(visible, jnp.exp(scores - largest[..., None]), 0.0)
    summed = jnp.sum(weights, axis=-1)
    partial_out = jnp.einsum(
        "hij,jhd->ihd",
        weights.astype(jnp.bfloat16),
        value_heads,
        preferred_element_type=jnp.float32,
    ).reshape(latents, channels)
    best, denom, combined = joined((largest.T, summed.T, partial_out), "seq", combine)
    attn_all = (combined / repeat_heads(denom)).astype(jnp.bfloat16)
    log_norm = best + jnp.log(denom)
    slab = out_proj.shape[0]
    attn_cols = lax.dynamic_slice_in_dim(attn_all, position * slab, slab, 1)
    proj_columns = lax.all_to_all(out_proj, "seq", split_axis=1, concat_axis=0, tiled=True)
    column_block = jnp.dot(attn_all, proj_columns, preferred_element_type=jnp.float32)
    hidden = lax.all_to_all(column_block, "seq", split_axis=0, concat_axis=1, tiled=True)
    inverse = lax.rsqrt(jnp.mean(hidden * hidden, axis=-1, keepdims=True) + epsilon)
    normed = (hidden * inverse * norm_gain).astype(jnp.bfloat16)
    logits = jnp.dot(normed, unembed, preferred_element_type=jnp.float32)
    log_total = jax.nn.logsumexp(logits, axis=-1, keepdims=True)
    onehot = (jnp.arange(logits.shape[1], dtype=jnp.int32)[None, :] == targets[0][:, None]).astype(
        jnp.float32
    )
    local_loss = jnp.sum(log_total[:, 0] - jnp.sum(logits * onehot, axis=-1))
    grad_logits = (loss_factor * (jnp.exp(logits - log_total) - onehot)).astype(jnp.bfloat16)
    grad_normed = lax.dot_general(
        grad_logits, unembed, (((1,), (1,)), ((), ())), preferred_element_type=jnp.float32
    )
    scaled = norm_gain * grad_normed
    grad_hidden = (
        inverse * scaled - hidden * inverse**3 * jnp.mean(hidden * scaled, axis=-1, keepdims=True)
    ).astype(jnp.bfloat16)
    grad_all = lax.all_gather(grad_hidden, "seq", axis=0, tiled=True)
    weight_part = lax.dot_general(
        attn_cols, grad_all, (((0,), (0,)), ((), ())), preferred_element_type=jnp.float32
    )
    grad_cols = lax.dot_general(
        grad_all, out_proj, (((1,), (1,)), ((), ())), preferred_element_type=jnp.float32
    ).astype(jnp.bfloat16)
    grad_attn = lax.all_gather(grad_cols, "seq", axis=1, tiled=True)
    grad_heads = grad_attn.reshape(latents, head_count, HD)
    product = grad_attn.astype(jnp.float32) * attn_all.astype(jnp.float32)
    delta = jnp.sum(product.reshape(latents, head_count, HD), axis=-1)
    probs = jnp.where(visible, jnp.exp(scores - log_norm.T[..., None]), 0.0)
    grad_probs = jnp.einsum(
        "ihd,jhd->hij", grad_heads, value_heads, preferred_element_type=jnp.float32
    )
    grad_scores = (probs * (grad_probs - delta.T[..., None])).astype(jnp.bfloat16)
    grad_values = (
        jnp.einsum(
            "hij,ihd->jhd",
            probs.astype(jnp.bfloat16),
            grad_heads,
            preferred_element_type=jnp.float32,
        )
        .reshape(tok_rows, channels)
        .astype(jnp.bfloat16)
    )
    grad_keys = (
        (
            jnp.einsum("hij,ihd->jhd", grad_scores, query_heads, preferred_element_type=jnp.float32)
            * softmax_scale
        )
        .reshape(tok_rows, channels)
        .astype(jnp.bfloat16)
    )
    terms = jnp.einsum("hij,jhd->ihd", grad_scores, key_heads, preferred_element_type=jnp.float32)
    grad_queries = lax.psum_scatter(
        (terms.reshape(lax.axis_size("seq") * own_rows, channels) * softmax_scale).astype(
            jnp.bfloat16
        ),
        "seq",
        scatter_dimension=0,
        tiled=True,
    )
    entries = channels * D
    weight_sum = lax.psum(weight_part.astype(jnp.bfloat16), "grp").astype(jnp.float32)
    loss_sum, square_sum = lax.psum((local_loss, jnp.sum(weight_sum * weight_sum)), "seq")
    proj_update = weight_sum * lax.rsqrt(square_sum / entries + epsilon)
    return (
        loss_sum.reshape(1),
        grad_queries[None],
        grad_keys[None],
        grad_values[None],
        proj_update,
    )


VMEM = pl.BlockSpec(memory_space=pltpu.VMEM)
SMEM = pl.BlockSpec(memory_space=pltpu.SMEM)
KEPT = object()
LOSS_ROWS = 16
TILE = 256
VMEM_LIMIT = 16 << 20
ROWS_T = (((1,), (1,)), ((), ()))
COLS_T = (((0,), (0,)), ((), ()))


def matmul(one, two, dims=(((1,), (0,)), ((), ()))):
    return lax.dot_general(one, two, dims, preferred_element_type=jnp.float32)


def kernel_call(kernel, in_specs, outs, scratch=(), flops=1 << 20, held=pltpu.VMEM):
    call = pl.pallas_call(
        kernel,
        in_specs=in_specs,
        out_specs=[VMEM if spec is KEPT else spec for _, _, spec in outs],
        out_shape=[
            (pltpu.VMEM if spec is KEPT else jax.ShapeDtypeStruct)(shape, dtype)
            for shape, dtype, spec in outs
        ],
        scratch_shapes=list(scratch),
        cost_estimate=pl.CostEstimate(flops=flops, bytes_accessed=0, transcendentals=0),
        compiler_params=pltpu.CompilerParams(vmem_limit_bytes=VMEM_LIMIT),
    )

    def placed(*operands):
        return call(
            *(
                pltpu.with_memory_space_constraint(operand, held)
                if spec is VMEM or held is pltpu.HBM
                else operand
                for spec, operand in zip(in_specs, operands)
            )
        )

    return placed


def head_cols(place, step):
    return pl.ds(pl.multiple_of((place[0] ^ step) * HD, HD), HD)


def pair_of(place, step):
    return (place[0] // 2 ^ step) * 2


def pack_kernel(place, targets, keys, values, queries, *pieces):
    tok = keys.shape[0]
    own = queries.shape[0]
    lanes = lax.broadcasted_iota(jnp.int32, (own, HD), 1)
    rows = lax.broadcasted_iota(jnp.int32, (own, HD), 0)
    wanted = jnp.zeros((own, HD), jnp.int32)
    for row in range(own):
        wanted = jnp.where(rows == row, targets[0, row], wanted)
    onehot = (lanes == wanted).astype(jnp.float32)
    for step, piece in enumerate(pieces):
        cols = head_cols(place, step)
        piece[0:tok, :] = keys[:, cols]
        piece[tok : 2 * tok, :] = values[:, cols]
        tail = jnp.concatenate([queries[:, cols].astype(jnp.float32), onehot], axis=0)
        piece[2 * tok : 2 * tok + 2 * own, :] = tail.astype(jnp.bfloat16)


def split_packed(packed, tok, own):
    heads = packed.shape[0]
    keys = packed[:, 0:tok, :].reshape(heads * tok, HD)
    values = packed[:, tok : 2 * tok, :].reshape(heads * tok, HD)
    queries = packed[:, 2 * tok : 2 * tok + own, :].astype(jnp.float32).reshape(heads * own, HD)
    return keys, values, queries.astype(jnp.bfloat16)


def visible_scores(keys, queries, positions):
    latents = queries.shape[0]
    length = keys.shape[0]
    diagonal = lax.broadcasted_iota(jnp.int32, (latents, latents), 0) == lax.broadcasted_iota(
        jnp.int32, (latents, latents), 1
    )
    last = jnp.sum(
        jnp.where(diagonal, positions[...].astype(jnp.float32), 0.0), axis=1, keepdims=True
    )
    places = lax.broadcasted_iota(jnp.int32, (latents, length), 1).astype(jnp.float32)
    scores = matmul(queries, keys, ROWS_T) * HD ** (-0.5)
    return scores, places <= last


def forward_kernel(place, positions, out_proj, gain, unembed, *refs, tok, own, count):
    pieces = refs[:count]
    packed, attn, log_norm, onehot, kept, sent, hidden = refs[count:]
    for step, piece in enumerate(pieces):
        packed[place[0] ^ step] = piece[...]
    keys, values, queries = split_packed(packed, tok, own)
    scores, visible = visible_scores(keys, queries, positions)
    best = jnp.max(jnp.where(visible, scores, -1e30), axis=-1, keepdims=True)
    weights = jnp.where(visible, jnp.exp(scores - best), 0.0)
    denom = jnp.sum(weights, axis=-1, keepdims=True)
    summed = matmul(weights.astype(jnp.bfloat16), values)
    attn[...] = (summed / denom).astype(jnp.bfloat16)
    log_norm[...] = jnp.broadcast_to(best + jnp.log(denom), log_norm.shape)
    half = kept.shape[0]
    mine = place[0] & 1
    pieces = half // own
    onehot[...] = (
        packed[pl.ds(mine * pieces, pieces), 2 * tok + own : 2 * tok + 2 * own, :]
        .astype(jnp.float32)
        .reshape(half, HD)
    )
    hidden[...] = matmul(attn[...], out_proj[...])
    kept[...] = hidden[pl.ds(pl.multiple_of(mine * half, half), half), :]
    sent[...] = hidden[pl.ds(pl.multiple_of((1 - mine) * half, half), half), :].astype(sent.dtype)


def exact_parts(value):
    high = value.astype(jnp.bfloat16).astype(jnp.float32)
    middle = (value - high).astype(jnp.bfloat16).astype(jnp.float32)
    return high, middle, value - high - middle


def loss_kernel(gain, unembed, onehot_ref, *refs):
    *parts, message, stats = refs
    half = onehot_ref.shape[0]
    hidden = parts[0][...].astype(jnp.float32)
    for part in parts[1:]:
        hidden = hidden + part[...].astype(jnp.float32)
    onehot = onehot_ref[...]
    inverse = lax.rsqrt(jnp.mean(hidden * hidden, axis=-1, keepdims=True) + epsilon)
    normed = (hidden * inverse * gain[...]).astype(jnp.bfloat16)
    logits = matmul(normed, unembed[...])
    top = jnp.max(logits, axis=-1, keepdims=True)
    log_total = top + jnp.log(jnp.sum(jnp.exp(logits - top), axis=-1, keepdims=True))
    losses = log_total - jnp.sum(logits * onehot, axis=-1, keepdims=True)
    total = jnp.broadcast_to(jnp.sum(losses, axis=0, keepdims=True), stats.shape)
    stats[...] = total
    grad_logits = (loss_factor * (jnp.exp(logits - log_total) - onehot)).astype(jnp.bfloat16)
    scaled = gain[...] * matmul(grad_logits, unembed[...], ROWS_T)
    mean = jnp.mean(hidden * scaled, axis=-1, keepdims=True)
    grad_hidden = (inverse * scaled - hidden * (inverse * inverse * inverse) * mean).astype(
        jnp.bfloat16
    )
    blocks = hidden.shape[1] // HD
    for block in range(blocks):
        message[block * half : (block + 1) * half, :] = grad_hidden[:, block * HD : (block + 1) * HD]
    row = lax.broadcasted_iota(jnp.int32, (LOSS_ROWS, HD), 0)
    high, middle, low = exact_parts(total)
    message[blocks * half :, :] = jnp.where(
        row == 0, high, jnp.where(row == 1, middle, jnp.where(row == 2, low, 0.0))
    ).astype(jnp.bfloat16)


def fill_rows(target, row, message, half):
    for block in range(target.shape[1] // HD):
        target[pl.ds(row, half), block * HD : (block + 1) * HD] = message[
            block * half : (block + 1) * half, :
        ]


def backward_kernel(
    place,
    positions,
    packed,
    out_proj,
    attn,
    log_norm,
    own_msg,
    pair_msg,
    *refs,
    tok,
    own,
):
    *messages, grads, grad_hidden = refs
    half = grad_hidden.shape[0] // 2
    mine = place[0] & 1
    fill_rows(grad_hidden, pl.multiple_of(mine * half, half), own_msg, half)
    fill_rows(grad_hidden, pl.multiple_of((1 - mine) * half, half), pair_msg, half)
    keys, values, queries = split_packed(packed, tok, own)
    scores, visible = visible_scores(keys, queries, positions)
    heads = packed.shape[0]
    grad_attn = matmul(grad_hidden[...], out_proj[...], ROWS_T).astype(jnp.bfloat16)
    delta = jnp.sum(
        grad_attn.astype(jnp.float32) * attn[...].astype(jnp.float32), axis=-1, keepdims=True
    )
    probs = jnp.where(visible, jnp.exp(scores - log_norm[:, 0:1]), 0.0)
    grad_probs = matmul(grad_attn, values, ROWS_T)
    grad_scores = (probs * (grad_probs - delta)).astype(jnp.bfloat16)
    grad_values = matmul(probs.astype(jnp.bfloat16), grad_attn, COLS_T).astype(jnp.bfloat16)
    scale = HD ** (-0.5)
    grad_keys = (matmul(grad_scores, queries, COLS_T) * scale).astype(jnp.bfloat16)
    grad_queries = matmul(grad_scores, keys) * scale
    grads[:, 0:tok, :] = grad_keys.reshape(heads, tok, HD)
    grads[:, tok : 2 * tok, :] = grad_values.reshape(heads, tok, HD)
    tail = grad_queries.reshape(heads, own, HD)
    grads[:, 2 * tok : 2 * tok + 2 * own, :] = jnp.concatenate([tail, tail], axis=1).astype(
        jnp.bfloat16
    )
    for step, message in enumerate(messages):
        message[...] = grads[pl.ds(pair_of(place, step), 2)]


def unpack_kernel(place, *refs):
    *messages, grad_queries, grad_keys, grad_values = refs
    tok = grad_keys.shape[0]
    own = grad_queries.shape[0]
    mine = place[0] & 1
    for index, message in enumerate(messages):
        pairs, side = index % (len(messages) // 2), index // (len(messages) // 2)
        source = pair_of(place, pairs) + (mine ^ side)
        cols = pl.ds(pl.multiple_of(source * HD, HD), HD)
        grad_keys[:, cols] = message[mine, 0:tok, :]
        grad_values[:, cols] = message[mine, tok : 2 * tok, :]
        grad_queries[:, cols] = message[mine, 2 * tok : 2 * tok + own, :]


def stack_kernel(*refs):
    *parts, stack = refs
    rows = parts[0].shape[0]
    for index, part in enumerate(parts):
        stack[index * rows : (index + 1) * rows, :] = part[...]


def total_kernel(loss_half, pair_msg, loss):
    other = pair_msg[pair_msg.shape[0] - LOSS_ROWS :, :].astype(jnp.float32)
    loss[...] = loss_half[...] + jnp.sum(other, axis=0, keepdims=True)


def weight_kernel(place, *refs, groups, seqs, entries):
    own_msgs = refs[:groups]
    pair_msgs = refs[groups : 2 * groups]
    attns = refs[2 * groups : 2 * groups + seqs]
    loss_in, update, loss, grad_hidden, attn_cols, total = refs[2 * groups + seqs :]
    loss[...] = loss_in[...]
    latents = grad_hidden.shape[0] // groups
    half = latents // 2
    mine = place[0] & 1
    for index in range(groups):
        first = index * latents
        fill_rows(
            grad_hidden, pl.multiple_of(first + mine * half, half), own_msgs[index], half
        )
        fill_rows(
            grad_hidden, pl.multiple_of(first + (1 - mine) * half, half), pair_msgs[index], half
        )
    for index in range(seqs):
        attn_cols[index * HD : (index + 1) * HD, :] = attns[index][...].T
    squares = jnp.zeros((8, TILE), jnp.float32)
    for tile in range(total.shape[1] // TILE):
        cols = slice(tile * TILE, (tile + 1) * TILE)
        part = matmul(attn_cols[...], grad_hidden[:, cols])
        total[:, cols] = part[0:HD]
        squares = squares + jnp.sum((part * part).reshape(seqs * HD // 8, 8, TILE), axis=0)
    square_sum = jnp.sum(jnp.sum(squares, axis=0, keepdims=True), axis=1, keepdims=True)
    update[...] = total[...] * lax.rsqrt(square_sum / entries + epsilon)


def body(hist_keys, hist_values, latent_queries, latent_pos, targets, out_proj, norm_gain, unembed):
    n_seq = lax.axis_size("seq")
    n_grp = lax.axis_size("grp")
    seq_keys = hist_keys[0]
    tok, channels = seq_keys.shape
    own = latent_queries.shape[1]
    latents = n_seq * own
    heads = channels // HD
    vocab = unembed.shape[1]
    if not (
        heads == n_seq
        and out_proj.shape[0] == HD
        and vocab == HD
        and tok % 16 == 0
        and own == 8
        and n_seq & (n_seq - 1) == 0
        and n_grp & (n_grp - 1) == 0
        and n_seq > 1
    ):
        return general_body(
            hist_keys, hist_values, latent_queries, latent_pos, targets, out_proj, norm_gain, unembed
        )
    bf16, f32 = jnp.bfloat16, jnp.float32
    half = latents // 2
    width = out_proj.shape[1]
    span = 2 * tok + 2 * own
    place = lax.axis_index("seq").reshape(1)
    steps = [[(i, i ^ step) for i in range(n_seq)] for step in range(1, n_seq)]
    swap = [(i, i ^ 1) for i in range(n_seq)]

    gain = norm_gain.reshape(1, width)
    pieces = kernel_call(
        pack_kernel,
        [SMEM, SMEM, VMEM, VMEM, VMEM],
        [((span, HD), bf16, KEPT)] * heads,
        held=pltpu.HBM,
    )(place, targets, seq_keys, hist_values[0], latent_queries[0])
    pieces = [pieces[0]] + [
        lax.ppermute(piece, "seq", perm) for piece, perm in zip(pieces[1:], steps)
    ]

    packed, attn, log_norm, onehot, kept, sent = kernel_call(
        partial(forward_kernel, tok=tok, own=own, count=heads),
        [SMEM] + [VMEM] * (4 + heads),
        [
            ((heads, span, HD), bf16, KEPT),
            ((latents, HD), bf16, KEPT),
            ((latents, HD), f32, KEPT),
            ((half, HD), f32, KEPT),
            ((half, width), f32, KEPT),
            ((half, width), bf16, KEPT),
        ],
        [pltpu.VMEM((latents, width), f32)],
    )(place, latent_pos, out_proj, gain, unembed, *pieces)
    pair_sum = (kept + lax.ppermute(sent, "seq", swap).astype(f32)).astype(bf16)
    chips = [[(i, i ^ step) for i in range(n_seq)] for step in range(2, n_seq, 2)]
    shifts = [[(i, i ^ step) for i in range(n_grp)] for step in range(1, n_grp)]
    parts = [pair_sum] + [lax.ppermute(pair_sum, "seq", perm) for perm in chips]
    attns = [attn] + [lax.ppermute(attn, "grp", perm) for perm in shifts]
    loss_call = kernel_call(
        loss_kernel,
        [VMEM] * (3 + len(parts)),
        [((width // HD * half + LOSS_ROWS, HD), bf16, KEPT), ((1, HD), f32, KEPT)],
        flops=1 << 26,
    )
    message, loss_half = loss_call(gain, unembed, onehot, *parts)
    pair_msg = lax.ppermute(message, "seq", swap)
    others = [lax.ppermute(message, "grp", perm) for perm in shifts]
    stack_call = kernel_call(stack_kernel, [VMEM] * n_grp, [((n_grp * latents, HD), bf16, KEPT)])
    (stack,) = stack_call(*attns)
    stacks = [stack] + [lax.ppermute(stack, "seq", perm) for perm in chips]
    backward = kernel_call(
        partial(backward_kernel, tok=tok, own=own),
        [SMEM] + [VMEM] * 7,
        [((2, span, HD), bf16, KEPT)] * (n_seq // 2),
        [pltpu.VMEM((heads, span, HD), bf16), pltpu.VMEM((latents, width), bf16)],
        flops=1 << 30,
    )
    grads = backward(place, latent_pos, packed, out_proj, attn, log_norm, message, pair_msg)
    others = lax.optimization_barrier((*others, grads[0]))[:-1]
    grads = [grads[0]] + [
        lax.ppermute(one, "seq", perm) for one, perm in zip(grads[1:], chips)
    ]
    grads = grads + [lax.ppermute(one, "seq", swap) for one in grads]
    total_call = kernel_call(total_kernel, [VMEM] * 2, [((1, HD), f32, KEPT)])
    (loss,) = total_call(loss_half, pair_msg)
    stacks = stacks + [lax.ppermute(one, "seq", swap) for one in stacks]
    pair_others = [lax.ppermute(other, "seq", swap) for other in others]
    weights_call = kernel_call(
        partial(weight_kernel, groups=n_grp, seqs=n_seq, entries=channels * width),
        [SMEM] + [VMEM] * (2 * n_grp + n_seq + 1),
        [((HD, width), f32, VMEM), ((1, HD), f32, VMEM)],
        [
            pltpu.VMEM((n_grp * latents, width), bf16),
            pltpu.VMEM((n_seq * HD, n_grp * latents), bf16),
            pltpu.VMEM((HD, width), f32),
        ],
    )
    proj_update, loss = weights_call(place, message, *others, pair_msg, *pair_others, *stacks, loss)
    unpack_call = kernel_call(
        unpack_kernel,
        [SMEM] + [VMEM] * heads,
        [
            ((own, channels), bf16, VMEM),
            ((tok, channels), bf16, VMEM),
            ((tok, channels), bf16, VMEM),
        ],
    )
    grad_queries, grad_keys, grad_values = unpack_call(place, *grads)
    loss_sum = loss[0, 0]
    return (
        loss_sum.reshape(1),
        grad_queries[None],
        grad_keys[None],
        grad_values[None],
        proj_update,
    )


def solution(mesh):
    placed = (
        P("grp", "seq", None),
        P("grp", "seq", None),
        P("grp", "seq", None),
        P("grp", None),
        P("grp", "seq"),
        P("seq", None),
        P(),
        P(),
    )
    return jax.shard_map(
        body,
        mesh=mesh,
        in_specs=placed,
        out_specs=(
            P("grp"),
            P("grp", "seq", None),
            P("grp", "seq", None),
            P("grp", "seq", None),
            P("seq", None),
        ),
        check_vma=False,
    )
```

```python
from functools import partial

import jax
import jax.numpy as jnp
from jax import lax
from jax.experimental import pallas as pl
from jax.experimental.pallas import tpu as pltpu
from jax.sharding import PartitionSpec as P


D = 2048
HD = 128


epsilon = 1e-06
loss_factor = 64.0


def joined(part, axis, combine):
    gathered = jax.tree.map(lambda a: lax.all_gather(a, axis), part)

    def take(source):
        return jax.tree.map(lambda a: lax.dynamic_index_in_dim(a, source, 0, False), gathered)

    return lax.fori_loop(
        1, lax.axis_size(axis), lambda source, state: combine(state, take(source)), take(0)
    )


def repeat_heads(stat):
    return jnp.repeat(stat, HD, axis=-1)


def combine(earlier, later):
    best = jnp.maximum(earlier[0], later[0])
    factor_one = jnp.exp(earlier[0] - best)
    factor_two = jnp.exp(later[0] - best)
    denom = earlier[1] * factor_one + later[1] * factor_two
    summed = earlier[2] * repeat_heads(factor_one) + later[2] * repeat_heads(factor_two)
    return (best, denom, summed)


def general_body(hist_keys, hist_values, latent_queries, latent_pos, targets, out_proj, norm_gain, unembed):
    softmax_scale = HD ** (-0.5)
    seq_keys = hist_keys[0]
    seq_values = hist_values[0]
    position = lax.axis_index("seq")
    tok_rows = seq_keys.shape[0]
    channels = seq_keys.shape[1]
    head_count = channels // HD
    own_rows = latent_queries.shape[1]
    queries = lax.all_gather(latent_queries[0], "seq", axis=0, tiled=True)
    latents = queries.shape[0]
    query_heads = queries.reshape(latents, head_count, HD)
    key_heads = seq_keys.reshape(tok_rows, head_count, HD)
    value_heads = seq_values.reshape(tok_rows, head_count, HD)
    places = position * tok_rows + jnp.arange(tok_rows, dtype=jnp.int32)
    visible = (places[None, :] <= latent_pos[0][:, None])[None]
    scores = (
        jnp.einsum("ihd,jhd->hij", query_heads, key_heads, preferred_element_type=jnp.float32)
        * softmax_scale
    )
    largest = jnp.max(jnp.where(visible, scores, -1e30), axis=-1)
    weights = jnp.where(visible, jnp.exp(scores - largest[..., None]), 0.0)
    summed = jnp.sum(weights, axis=-1)
    partial_out = jnp.einsum(
        "hij,jhd->ihd",
        weights.astype(jnp.bfloat16),
        value_heads,
        preferred_element_type=jnp.float32,
    ).reshape(latents, channels)
    best, denom, combined = joined((largest.T, summed.T, partial_out), "seq", combine)
    attn_all = (combined / repeat_heads(denom)).astype(jnp.bfloat16)
    log_norm = best + jnp.log(denom)
    slab = out_proj.shape[0]
    attn_cols = lax.dynamic_slice_in_dim(attn_all, position * slab, slab, 1)
    proj_columns = lax.all_to_all(out_proj, "seq", split_axis=1, concat_axis=0, tiled=True)
    column_block = jnp.dot(attn_all, proj_columns, preferred_element_type=jnp.float32)
    hidden = lax.all_to_all(column_block, "seq", split_axis=0, concat_axis=1, tiled=True)
    inverse = lax.rsqrt(jnp.mean(hidden * hidden, axis=-1, keepdims=True) + epsilon)
    normed = (hidden * inverse * norm_gain).astype(jnp.bfloat16)
    logits = jnp.dot(normed, unembed, preferred_element_type=jnp.float32)
    log_total = jax.nn.logsumexp(logits, axis=-1, keepdims=True)
    onehot = (jnp.arange(logits.shape[1], dtype=jnp.int32)[None, :] == targets[0][:, None]).astype(
        jnp.float32
    )
    local_loss = jnp.sum(log_total[:, 0] - jnp.sum(logits * onehot, axis=-1))
    grad_logits = (loss_factor * (jnp.exp(logits - log_total) - onehot)).astype(jnp.bfloat16)
    grad_normed = lax.dot_general(
        grad_logits, unembed, (((1,), (1,)), ((), ())), preferred_element_type=jnp.float32
    )
    scaled = norm_gain * grad_normed
    grad_hidden = (
        inverse * scaled - hidden * inverse**3 * jnp.mean(hidden * scaled, axis=-1, keepdims=True)
    ).astype(jnp.bfloat16)
    grad_all = lax.all_gather(grad_hidden, "seq", axis=0, tiled=True)
    weight_part = lax.dot_general(
        attn_cols, grad_all, (((0,), (0,)), ((), ())), preferred_element_type=jnp.float32
    )
    grad_cols = lax.dot_general(
        grad_all, out_proj, (((1,), (1,)), ((), ())), preferred_element_type=jnp.float32
    ).astype(jnp.bfloat16)
    grad_attn = lax.all_gather(grad_cols, "seq", axis=1, tiled=True)
    grad_heads = grad_attn.reshape(latents, head_count, HD)
    product = grad_attn.astype(jnp.float32) * attn_all.astype(jnp.float32)
    delta = jnp.sum(product.reshape(latents, head_count, HD), axis=-1)
    probs = jnp.where(visible, jnp.exp(scores - log_norm.T[..., None]), 0.0)
    grad_probs = jnp.einsum(
        "ihd,jhd->hij", grad_heads, value_heads, preferred_element_type=jnp.float32
    )
    grad_scores = (probs * (grad_probs - delta.T[..., None])).astype(jnp.bfloat16)
    grad_values = (
        jnp.einsum(
            "hij,ihd->jhd",
            probs.astype(jnp.bfloat16),
            grad_heads,
            preferred_element_type=jnp.float32,
        )
        .reshape(tok_rows, channels)
        .astype(jnp.bfloat16)
    )
    grad_keys = (
        (
            jnp.einsum("hij,ihd->jhd", grad_scores, query_heads, preferred_element_type=jnp.float32)
            * softmax_scale
        )
        .reshape(tok_rows, channels)
        .astype(jnp.bfloat16)
    )
    terms = jnp.einsum("hij,jhd->ihd", grad_scores, key_heads, preferred_element_type=jnp.float32)
    grad_queries = lax.psum_scatter(
        (terms.reshape(lax.axis_size("seq") * own_rows, channels) * softmax_scale).astype(
            jnp.bfloat16
        ),
        "seq",
        scatter_dimension=0,
        tiled=True,
    )
    entries = channels * D
    weight_sum = lax.psum(weight_part.astype(jnp.bfloat16), "grp").astype(jnp.float32)
    loss_sum, square_sum = lax.psum((local_loss, jnp.sum(weight_sum * weight_sum)), "seq")
    proj_update = weight_sum * lax.rsqrt(square_sum / entries + epsilon)
    return (
        loss_sum.reshape(1),
        grad_queries[None],
        grad_keys[None],
        grad_values[None],
        proj_update,
    )


VMEM = pl.BlockSpec(memory_space=pltpu.VMEM)
SMEM = pl.BlockSpec(memory_space=pltpu.SMEM)
KEPT = object()
LOSS_ROWS = 16
TILE = 256
VMEM_LIMIT = 16 << 20
ROWS_T = (((1,), (1,)), ((), ()))
COLS_T = (((0,), (0,)), ((), ()))


def matmul(one, two, dims=(((1,), (0,)), ((), ()))):
    return lax.dot_general(one, two, dims, preferred_element_type=jnp.float32)


def kernel_call(kernel, in_specs, outs, scratch=(), flops=1 << 20, held=pltpu.VMEM):
    call = pl.pallas_call(
        kernel,
        in_specs=in_specs,
        out_specs=[VMEM if spec is KEPT else spec for _, _, spec in outs],
        out_shape=[
            (pltpu.VMEM if spec is KEPT else jax.ShapeDtypeStruct)(shape, dtype)
            for shape, dtype, spec in outs
        ],
        scratch_shapes=list(scratch),
        cost_estimate=pl.CostEstimate(flops=flops, bytes_accessed=0, transcendentals=0),
        compiler_params=pltpu.CompilerParams(vmem_limit_bytes=VMEM_LIMIT),
    )

    def placed(*operands):
        return call(
            *(
                pltpu.with_memory_space_constraint(operand, held)
                if spec is VMEM or held is pltpu.HBM
                else operand
                for spec, operand in zip(in_specs, operands)
            )
        )

    return placed


def head_cols(place, step):
    return pl.ds(pl.multiple_of((place[0] ^ step) * HD, HD), HD)


def pair_of(place, step):
    return (place[0] // 2 ^ step) * 2


def pack_kernel(place, targets, keys, values, queries, *pieces):
    tok = keys.shape[0]
    own = queries.shape[0]
    lanes = lax.broadcasted_iota(jnp.int32, (own, HD), 1)
    rows = lax.broadcasted_iota(jnp.int32, (own, HD), 0)
    wanted = jnp.zeros((own, HD), jnp.int32)
    for row in range(own):
        wanted = jnp.where(rows == row, targets[0, row], wanted)
    onehot = (lanes == wanted).astype(jnp.float32)
    for step, piece in enumerate(pieces):
        cols = head_cols(place, step)
        piece[0:tok, :] = keys[:, cols]
        piece[tok : 2 * tok, :] = values[:, cols]
        tail = jnp.concatenate([queries[:, cols].astype(jnp.float32), onehot], axis=0)
        piece[2 * tok : 2 * tok + 2 * own, :] = tail.astype(jnp.bfloat16)


def split_packed(packed, tok, own):
    heads = packed.shape[0]
    keys = packed[:, 0:tok, :].reshape(heads * tok, HD)
    values = packed[:, tok : 2 * tok, :].reshape(heads * tok, HD)
    queries = packed[:, 2 * tok : 2 * tok + own, :].astype(jnp.float32).reshape(heads * own, HD)
    return keys, values, queries.astype(jnp.bfloat16)


def visible_scores(keys, queries, positions):
    latents = queries.shape[0]
    length = keys.shape[0]
    diagonal = lax.broadcasted_iota(jnp.int32, (latents, latents), 0) == lax.broadcasted_iota(
        jnp.int32, (latents, latents), 1
    )
    last = jnp.sum(
        jnp.where(diagonal, positions[...].astype(jnp.float32), 0.0), axis=1, keepdims=True
    )
    places = lax.broadcasted_iota(jnp.int32, (latents, length), 1).astype(jnp.float32)
    scores = matmul(queries, keys, ROWS_T) * HD ** (-0.5)
    return scores, places <= last


def forward_kernel(place, positions, out_proj, gain, unembed, *refs, tok, own, count):
    pieces = refs[:count]
    packed, attn, log_norm, onehot, kept, sent, hidden = refs[count:]
    for step, piece in enumerate(pieces):
        packed[place[0] ^ step] = piece[...]
    keys, values, queries = split_packed(packed, tok, own)
    scores, visible = visible_scores(keys, queries, positions)
    best = jnp.max(jnp.where(visible, scores, -1e30), axis=-1, keepdims=True)
    weights = jnp.where(visible, jnp.exp(scores - best), 0.0)
    denom = jnp.sum(weights, axis=-1, keepdims=True)
    summed = matmul(weights.astype(jnp.bfloat16), values)
    attn[...] = (summed / denom).astype(jnp.bfloat16)
    log_norm[...] = jnp.broadcast_to(best + jnp.log(denom), log_norm.shape)
    half = kept.shape[0]
    mine = place[0] & 1
    pieces = half // own
    onehot[...] = (
        packed[pl.ds(mine * pieces, pieces), 2 * tok + own : 2 * tok + 2 * own, :]
        .astype(jnp.float32)
        .reshape(half, HD)
    )
    hidden[...] = matmul(attn[...], out_proj[...])
    kept[...] = hidden[pl.ds(pl.multiple_of(mine * half, half), half), :]
    sent[...] = hidden[pl.ds(pl.multiple_of((1 - mine) * half, half), half), :].astype(sent.dtype)


def exact_parts(value):
    high = value.astype(jnp.bfloat16).astype(jnp.float32)
    middle = (value - high).astype(jnp.bfloat16).astype(jnp.float32)
    return high, middle, value - high - middle


def loss_kernel(gain, unembed, onehot_ref, *refs):
    *parts, message, stats = refs
    half = onehot_ref.shape[0]
    hidden = parts[0][...].astype(jnp.float32)
    for part in parts[1:]:
        hidden = hidden + part[...].astype(jnp.float32)
    onehot = onehot_ref[...]
    inverse = lax.rsqrt(jnp.mean(hidden * hidden, axis=-1, keepdims=True) + epsilon)
    normed = (hidden * inverse * gain[...]).astype(jnp.bfloat16)
    logits = matmul(normed, unembed[...])
    top = jnp.max(logits, axis=-1, keepdims=True)
    log_total = top + jnp.log(jnp.sum(jnp.exp(logits - top), axis=-1, keepdims=True))
    losses = log_total - jnp.sum(logits * onehot, axis=-1, keepdims=True)
    total = jnp.broadcast_to(jnp.sum(losses, axis=0, keepdims=True), stats.shape)
    stats[...] = total
    grad_logits = (loss_factor * (jnp.exp(logits - log_total) - onehot)).astype(jnp.bfloat16)
    scaled = gain[...] * matmul(grad_logits, unembed[...], ROWS_T)
    mean = jnp.mean(hidden * scaled, axis=-1, keepdims=True)
    grad_hidden = (inverse * scaled - hidden * (inverse * inverse * inverse) * mean).astype(
        jnp.bfloat16
    )
    blocks = hidden.shape[1] // HD
    for block in range(blocks):
        message[block * half : (block + 1) * half, :] = grad_hidden[:, block * HD : (block + 1) * HD]
    row = lax.broadcasted_iota(jnp.int32, (LOSS_ROWS, HD), 0)
    high, middle, low = exact_parts(total)
    message[blocks * half :, :] = jnp.where(
        row == 0, high, jnp.where(row == 1, middle, jnp.where(row == 2, low, 0.0))
    ).astype(jnp.bfloat16)


def fill_rows(target, row, message, half):
    for block in range(target.shape[1] // HD):
        target[pl.ds(row, half), block * HD : (block + 1) * HD] = message[
            block * half : (block + 1) * half, :
        ]


def backward_kernel(
    place,
    positions,
    packed,
    out_proj,
    attn,
    log_norm,
    own_msg,
    pair_msg,
    *refs,
    tok,
    own,
):
    *messages, grads, grad_hidden = refs
    half = grad_hidden.shape[0] // 2
    mine = place[0] & 1
    fill_rows(grad_hidden, pl.multiple_of(mine * half, half), own_msg, half)
    fill_rows(grad_hidden, pl.multiple_of((1 - mine) * half, half), pair_msg, half)
    keys, values, queries = split_packed(packed, tok, own)
    scores, visible = visible_scores(keys, queries, positions)
    heads = packed.shape[0]
    grad_attn = matmul(grad_hidden[...], out_proj[...], ROWS_T).astype(jnp.bfloat16)
    delta = jnp.sum(
        grad_attn.astype(jnp.float32) * attn[...].astype(jnp.float32), axis=-1, keepdims=True
    )
    probs = jnp.where(visible, jnp.exp(scores - log_norm[:, 0:1]), 0.0)
    grad_probs = matmul(grad_attn, values, ROWS_T)
    grad_scores = (probs * (grad_probs - delta)).astype(jnp.bfloat16)
    grad_values = matmul(probs.astype(jnp.bfloat16), grad_attn, COLS_T).astype(jnp.bfloat16)
    scale = HD ** (-0.5)
    grad_keys = (matmul(grad_scores, queries, COLS_T) * scale).astype(jnp.bfloat16)
    grad_queries = matmul(grad_scores, keys) * scale
    grads[:, 0:tok, :] = grad_keys.reshape(heads, tok, HD)
    grads[:, tok : 2 * tok, :] = grad_values.reshape(heads, tok, HD)
    tail = grad_queries.reshape(heads, own, HD)
    grads[:, 2 * tok : 2 * tok + 2 * own, :] = jnp.concatenate([tail, tail], axis=1).astype(
        jnp.bfloat16
    )
    for step, message in enumerate(messages):
        message[...] = grads[pl.ds(pair_of(place, step), 2)]


def unpack_kernel(place, *refs):
    *messages, grad_queries, grad_keys, grad_values = refs
    tok = grad_keys.shape[0]
    own = grad_queries.shape[0]
    mine = place[0] & 1
    for index, message in enumerate(messages):
        pairs, side = index % (len(messages) // 2), index // (len(messages) // 2)
        source = pair_of(place, pairs) + (mine ^ side)
        cols = pl.ds(pl.multiple_of(source * HD, HD), HD)
        grad_keys[:, cols] = message[mine, 0:tok, :]
        grad_values[:, cols] = message[mine, tok : 2 * tok, :]
        grad_queries[:, cols] = message[mine, 2 * tok : 2 * tok + own, :]


def stack_kernel(*refs):
    *parts, stack = refs
    rows = parts[0].shape[0]
    for index, part in enumerate(parts):
        stack[index * rows : (index + 1) * rows, :] = part[...]


def total_kernel(loss_half, pair_msg, loss):
    other = pair_msg[pair_msg.shape[0] - LOSS_ROWS :, :].astype(jnp.float32)
    loss[...] = loss_half[...] + jnp.sum(other, axis=0, keepdims=True)


def weight_kernel(place, *refs, groups, seqs):
    own_msgs = refs[:groups]
    pair_msgs = refs[groups : 2 * groups]
    attns = refs[2 * groups : 2 * groups + seqs]
    total, square_sums, grad_hidden, attn_cols = refs[2 * groups + seqs :]
    latents = grad_hidden.shape[0] // groups
    half = latents // 2
    mine = place[0] & 1
    for index in range(groups):
        first = index * latents
        fill_rows(
            grad_hidden, pl.multiple_of(first + mine * half, half), own_msgs[index], half
        )
        fill_rows(
            grad_hidden, pl.multiple_of(first + (1 - mine) * half, half), pair_msgs[index], half
        )
    for index in range(seqs):
        attn_cols[index * HD : (index + 1) * HD, :] = attns[index][...].T
    squares = jnp.zeros((8, TILE), jnp.float32)
    for tile in range(total.shape[1] // TILE):
        cols = slice(tile * TILE, (tile + 1) * TILE)
        part = matmul(attn_cols[...], grad_hidden[:, cols])
        total[:, cols] = part[0:HD]
        squares = squares + jnp.sum((part * part).reshape(seqs * HD // 8, 8, TILE), axis=0)
    square_sum = jnp.sum(jnp.sum(squares, axis=0, keepdims=True), axis=1, keepdims=True)
    square_sums[...] = jnp.broadcast_to(square_sum, square_sums.shape)


def scale_kernel(total, squares, other_squares, loss_in, update, loss, *, entries):
    square_sum = squares[:, 0:1] + other_squares[:, 0:1]
    update[...] = total[...] * lax.rsqrt(square_sum / entries + epsilon)
    loss[...] = loss_in[...]


def body(hist_keys, hist_values, latent_queries, latent_pos, targets, out_proj, norm_gain, unembed):
    n_seq = lax.axis_size("seq")
    n_grp = lax.axis_size("grp")
    seq_keys = hist_keys[0]
    tok, channels = seq_keys.shape
    own = latent_queries.shape[1]
    latents = n_seq * own
    heads = channels // HD
    vocab = unembed.shape[1]
    if not (
        heads == n_seq
        and out_proj.shape[0] == HD
        and vocab == HD
        and tok % 16 == 0
        and own == 8
        and n_seq & (n_seq - 1) == 0
        and n_grp & (n_grp - 1) == 0
        and n_seq > 1
    ):
        return general_body(
            hist_keys, hist_values, latent_queries, latent_pos, targets, out_proj, norm_gain, unembed
        )
    bf16, f32 = jnp.bfloat16, jnp.float32
    half = latents // 2
    width = out_proj.shape[1]
    span = 2 * tok + 2 * own
    place = lax.axis_index("seq").reshape(1)
    steps = [[(i, i ^ step) for i in range(n_seq)] for step in range(1, n_seq)]
    swap = [(i, i ^ 1) for i in range(n_seq)]

    gain = norm_gain.reshape(1, width)
    pieces = kernel_call(
        pack_kernel,
        [SMEM, SMEM, VMEM, VMEM, VMEM],
        [((span, HD), bf16, KEPT)] * heads,
        held=pltpu.HBM,
    )(place, targets, seq_keys, hist_values[0], latent_queries[0])
    pieces = [pieces[0]] + [
        lax.ppermute(piece, "seq", perm) for piece, perm in zip(pieces[1:], steps)
    ]

    packed, attn, log_norm, onehot, kept, sent = kernel_call(
        partial(forward_kernel, tok=tok, own=own, count=heads),
        [SMEM] + [VMEM] * (4 + heads),
        [
            ((heads, span, HD), bf16, KEPT),
            ((latents, HD), bf16, KEPT),
            ((latents, HD), f32, KEPT),
            ((half, HD), f32, KEPT),
            ((half, width), f32, KEPT),
            ((half, width), bf16, KEPT),
        ],
        [pltpu.VMEM((latents, width), f32)],
    )(place, latent_pos, out_proj, gain, unembed, *pieces)
    pair_sum = (kept + lax.ppermute(sent, "seq", swap).astype(f32)).astype(bf16)
    chips = [[(i, i ^ step) for i in range(n_seq)] for step in range(2, n_seq, 2)]
    shifts = [[(i, i ^ step) for i in range(n_grp)] for step in range(1, n_grp)]
    parts = [pair_sum] + [lax.ppermute(pair_sum, "seq", perm) for perm in chips]
    attns = [attn] + [lax.ppermute(attn, "grp", perm) for perm in shifts]
    loss_call = kernel_call(
        loss_kernel,
        [VMEM] * (3 + len(parts)),
        [((width // HD * half + LOSS_ROWS, HD), bf16, KEPT), ((1, HD), f32, KEPT)],
        flops=1 << 26,
    )
    message, loss_half = loss_call(gain, unembed, onehot, *parts)
    pair_msg = lax.ppermute(message, "seq", swap)
    others = [lax.ppermute(message, "grp", perm) for perm in shifts]
    stack_call = kernel_call(stack_kernel, [VMEM] * n_grp, [((n_grp * latents, HD), bf16, KEPT)])
    (stack,) = stack_call(*attns)
    stacks = [stack] + [lax.ppermute(stack, "seq", perm) for perm in chips]
    backward = kernel_call(
        partial(backward_kernel, tok=tok, own=own),
        [SMEM] + [VMEM] * 7,
        [((2, span, HD), bf16, KEPT)] * (n_seq // 2),
        [pltpu.VMEM((heads, span, HD), bf16), pltpu.VMEM((latents, width), bf16)],
        flops=1 << 30,
    )
    grads = backward(place, latent_pos, packed, out_proj, attn, log_norm, message, pair_msg)
    others = lax.optimization_barrier((*others, grads[0]))[:-1]
    grads = [grads[0]] + [
        lax.ppermute(one, "seq", perm) for one, perm in zip(grads[1:], chips)
    ]
    grads = grads + [lax.ppermute(one, "seq", swap) for one in grads]
    total_call = kernel_call(total_kernel, [VMEM] * 2, [((1, HD), f32, KEPT)])
    (loss,) = total_call(loss_half, pair_msg)
    pair_others = [lax.ppermute(other, "seq", swap) for other in others]
    weights_call = kernel_call(
        partial(weight_kernel, groups=n_grp, seqs=n_seq // 2),
        [SMEM] + [VMEM] * (2 * n_grp + n_seq // 2),
        [((HD, width), f32, KEPT), ((1, HD), f32, KEPT)],
        [
            pltpu.VMEM((n_grp * latents, width), bf16),
            pltpu.VMEM((n_seq // 2 * HD, n_grp * latents), bf16),
        ],
    )
    total, squares = weights_call(place, message, *others, pair_msg, *pair_others, *stacks)
    other_squares = lax.ppermute(squares, "seq", swap)
    unpack_call = kernel_call(
        unpack_kernel,
        [SMEM] + [VMEM] * heads,
        [
            ((own, channels), bf16, VMEM),
            ((tok, channels), bf16, VMEM),
            ((tok, channels), bf16, VMEM),
        ],
    )
    grad_queries, grad_keys, grad_values = unpack_call(place, *grads)
    scale_call = kernel_call(
        partial(scale_kernel, entries=channels * width),
        [VMEM] * 4,
        [((HD, width), f32, VMEM), ((1, HD), f32, VMEM)],
    )
    proj_update, loss = scale_call(total, squares, other_squares, loss)
    loss_sum = loss[0, 0]
    return (
        loss_sum.reshape(1),
        grad_queries[None],
        grad_keys[None],
        grad_values[None],
        proj_update,
    )


def solution(mesh):
    placed = (
        P("grp", "seq", None),
        P("grp", "seq", None),
        P("grp", "seq", None),
        P("grp", None),
        P("grp", "seq"),
        P("seq", None),
        P(),
        P(),
    )
    return jax.shard_map(
        body,
        mesh=mesh,
        in_specs=placed,
        out_specs=(
            P("grp"),
            P("grp", "seq", None),
            P("grp", "seq", None),
            P("grp", "seq", None),
            P("seq", None),
        ),
        check_vma=False,
    )
```
